32 devices in a mesh: band: 8 (over y, x, core), chan: 4 (over z).
Axes of the slice: x: 2, y: 2, z: 4, core: 2. Of those that a mesh axis runs over, the one named last changes fastest.
Arguments:
- cells_next: bfloat16 [16384, 1024], P('band', 'chan'), may hold values from -6 to 6
- node_embed: bfloat16 [2048, 1024], P('band', 'chan'), may hold values from -6 to 6
- enc_mix: bfloat16 [1024, 1024], P(None, 'chan'), may hold values from -0.1875 to 0.1875
- out_cotangent: bfloat16 [16384, 1024], P('band', 'chan'), may hold values from -6 to 6
- decoded_saved: bfloat16 [16384, 1024], P('band', 'chan'), may hold values from -6 to 6
- dec_proj: bfloat16 [1024, 1024], P(None, 'chan'), may hold values from -0.1875 to 0.1875
- tile_source: int32 [16, 16], replicated, may hold values from 0 to 127, as said below
- tile_codes: int32 [16, 16, 128, 128], P('band'), may hold values from 0 to 65535
Outputs:
- hidden_nodes: bfloat16 [2048, 1024], P('band', 'chan')
- node_grad: bfloat16 [2048, 1024], P('band', 'chan')
- w_dec_grad: float32 [1024, 1024], P('band', 'chan')
The draws below stay inside these ranges and needn't reach their ends.
Inputs may be any that keep to these rules, and one draw needn't show every extreme that they name: `tile_source`: each entry is a cell block; cell block c lies in band c // 16 and node block n in band n // 2. The cell blocks of a node block's tiles lie within 3 bands of its own. Of the 32 tiles of one band's node blocks, exactly 8 read that band itself and at most 8 read any other one band.
All inputs are finite; a program needn't handle non-finite values.
Results may differ from the reference program's by a relative error of at most 0.0049.
Values may be sent and summed in bfloat16 or wider, within the bound.
A program may use at most 64 MiB of HBM per device.

```python
import jax
import jax.numpy as jnp
from jax import lax

D = 1024
BLK = 128
K = 16
R = 3
CB_DEV = 16
NB_DEV = 2
CAP = 8
NODE_BLOCKS = 16
CELLS = 16384
NODES = 2048


def draw_tile_source(key, part):
    band_total = NODE_BLOCKS // NB_DEV
    tile_total = NB_DEV * K
    pool_size = 2 * R * CAP

    def one_band(band_key, owner):
        score_key, shuffle_key, local_key = jax.random.split(band_key, 3)
        tokens = jnp.arange(pool_size, dtype=jnp.int32)
        neighbour = tokens // CAP
        offset = jnp.where(neighbour < R, neighbour - R, neighbour - R + 1)
        source = owner + offset
        usable = (source >= 0) & (source < band_total)
        scores = jax.random.randint(score_key, (pool_size,), 0, 1 << 20, dtype=jnp.int32) * pool_size + tokens
        scores = jnp.where(usable, scores, (1 << 30) + tokens)
        ranking = jnp.argsort(scores)
        picked = source[ranking[:tile_total - CAP]]
        bands_drawn = jnp.concatenate([jnp.full((CAP,), owner, jnp.int32), picked.astype(jnp.int32)])
        shuffle = jax.random.permutation(shuffle_key, tile_total)
        local_block = jax.random.randint(local_key, (tile_total,), 0, CB_DEV, dtype=jnp.int32)
        return (bands_drawn[shuffle] * CB_DEV + local_block).reshape(NB_DEV, K)
    band_keys = jax.random.split(key, band_total)
    drawn = jax.vmap(one_band)(band_keys, jnp.arange(band_total, dtype=jnp.int32))
    return drawn.reshape(band_total * NB_DEV, K).astype(jnp.int32)


def plant(array, rng, smallest, high):
    extent = array.shape
    place = [jax.random.randint(jax.random.fold_in(rng, axis), (), 0, extent[axis]) for axis in range(len(extent))]
    array = array.at[tuple(place)].set(smallest)
    longest = extent.index(max(extent))
    place[longest] = (place[longest] + 1) % extent[longest]
    return array.at[tuple(place)].set(high)


def spiked(result, own_key, source, target, shards_of, factor):
    owner, partner = [(jnp.arange(result.shape[position]) // (result.shape[position] // shards_of)).reshape([-1 if axis == position else 1 for axis in range(result.ndim)]) for position in (source, target)]
    chosen = jax.random.permutation(own_key, shards_of)[partner]
    strong = (owner == chosen) | (owner == (partner + shards_of // 2) % shards_of)
    return jnp.where(strong, factor * result, result)


def shard_levels(own_key, shape, shards, smallest, top_value):
    level = 1.0
    for axis_at, parts in shards:
        steps = jax.random.uniform(jax.random.fold_in(jax.random.fold_in(own_key, 6), axis_at), (parts,), jnp.float32, smallest / len(shards), top_value / len(shards))
        level = level * jnp.repeat(jnp.exp(steps), shape[axis_at] // parts).reshape((-1,) + (1,) * (len(shape) - 1 - axis_at))
    return level


def noise(rng, shape, scale, reach, shards=(), kind=jnp.bfloat16):
    values = scale * jax.random.normal(rng, shape, jnp.float32)
    if shards:
        values = values * shard_levels(rng, shape, shards, -0.22, 0.18)
    return jnp.clip(values, -reach, reach).astype(kind)


def heavy_noise(stream_key, extent, spread, limit, cuts, heavy, held_as=jnp.bfloat16):
    entries = spread * jax.random.normal(stream_key, extent, jnp.float32)
    if cuts:
        entries = entries * shard_levels(stream_key, extent, cuts, -0.22, 0.18)
    return jnp.clip(spiked(entries, jax.random.fold_in(stream_key, 3), *heavy), -limit, limit).astype(held_as)


def setup_inputs(seed: int = 0) -> dict:
    arg_keys = jax.random.split(jax.random.key(seed), 9)
    cells_next = noise(arg_keys[0], (CELLS, D), 1.0, 6.0, ((0, 8), (1, 4)))
    node_embed = noise(arg_keys[1], (NODES, D), 1.0, 6.0, ((0, 8), (1, 4)))
    enc_mix = noise(arg_keys[2], (D, D), D ** -0.5, 0.1875, ((1, 4),))
    out_cotangent = heavy_noise(arg_keys[3], (CELLS, D), 1.0, 6.0, ((0, 8), (1, 4)), (0, 1, 8, 2.0))
    decoded_saved = noise(arg_keys[4], (CELLS, D), 1.0, 6.0, ((0, 8), (1, 4)))
    dec_proj = noise(arg_keys[5], (D, D), D ** -0.5, 0.1875, ((1, 4),))
    tile_source = draw_tile_source(jax.random.fold_in(arg_keys[8], 71), 0)
    tile_codes = plant(jax.random.randint(arg_keys[7], (NODE_BLOCKS, K, BLK, BLK), 0, 65536), jax.random.fold_in(arg_keys[7], 1), 0, 65535).astype(jnp.int32)
    return {"cells_next": cells_next, "node_embed": node_embed, "enc_mix": enc_mix, "out_cotangent": out_cotangent, "decoded_saved": decoded_saved, "dec_proj": dec_proj, "tile_source": tile_source, "tile_codes": tile_codes}


def split_codes(code_words):
    low_codes = (code_words % 256 - 128).astype(jnp.bfloat16)
    high_codes = (code_words // 256 - 128).astype(jnp.bfloat16)
    return low_codes, high_codes


def reference(cells_next, node_embed, enc_mix, out_cotangent, decoded_saved, dec_proj, tile_source, tile_codes):
    tile_scale = (3.0 / (K * BLK)) ** 0.5 / 128.0
    channels = cells_next.shape[1]
    cotangent_wide = out_cotangent.astype(jnp.float32)
    cell_grad = jnp.dot(cotangent_wide, dec_proj.astype(jnp.float32), preferred_element_type=jnp.float32).astype(jnp.bfloat16)
    cell_blocks = cells_next.reshape(-1, BLK, channels)
    grad_blocks = cell_grad.reshape(-1, BLK, channels)

    def per_block(inputs):
        sources, code_words = inputs
        enc_tile, dec_tile = split_codes(code_words)
        gathered = cell_blocks[sources].astype(jnp.float32)
        aggregate = jnp.einsum("kab,kbd->ad", enc_tile.astype(jnp.float32), gathered) * tile_scale
        grad_rows = grad_blocks[sources].astype(jnp.float32)
        node_part = jnp.einsum("kab,kbd->ad", dec_tile.astype(jnp.float32), grad_rows) * tile_scale
        return aggregate.astype(jnp.bfloat16), node_part.astype(jnp.bfloat16)

    agg_blocks, node_blocks = lax.map(per_block, (tile_source, tile_codes))
    aggregate = agg_blocks.reshape(-1, channels)
    mixed_rows = jnp.dot(aggregate, enc_mix, preferred_element_type=jnp.float32)
    hidden_nodes = (node_embed.astype(jnp.float32) + jax.nn.silu(mixed_rows)).astype(jnp.bfloat16)
    node_grad = node_blocks.reshape(-1, channels)
    w_dec_grad = jnp.dot(cotangent_wide.T, decoded_saved.astype(jnp.float32), preferred_element_type=jnp.float32) * (CELLS ** -0.5)
    return hidden_nodes, node_grad, w_dec_grad
```

```python
import functools

import jax
import jax.numpy as jnp
from jax import lax
from jax.experimental import pallas as pl
from jax.experimental.pallas import tpu as pltpu
from jax.sharding import PartitionSpec as P

R = 3
CAP = 8
SEND_ORDER = [3, 2, -2, -1, -3, 1]
MATE = -1
PAIRED = {v for v in range(-R, R + 1) if v not in (0, MATE) and -v - 1 not in (0, MATE) and -R <= -v - 1 <= R}
SERVE_AT = {-3: 2.6, 2: 4.6, -2: 6.6, 1: 7.6, 3: 7.7, -1: 7.8}
JOIN_AT = {-3: 4.7, 2: 4.8, -2: 7.9, 1: 8.0}
GATHER_AT = 10.6
NCH = 8
NH = 6
LEAD = NCH // 2
MESH = pl.DeviceIdType.MESH
F32 = jnp.float32
BF16 = jnp.bfloat16


def tables_for(tile_source, me, nb, tiles, nodes, cb):
    rows = tile_source.reshape(nb, tiles)
    offs = jnp.arange(-R, R + 1, dtype=jnp.int32) * (1 - 2 * (me % 2))
    served = rows[jnp.clip(me - offs, 0, nb - 1)]
    order = jnp.arange(tiles, dtype=jnp.int32)
    before = order[None, :] < order[:, None]

    def onehot(sel):
        rank = jnp.sum((sel[:, None, :] & before[None]).astype(jnp.int32), axis=2)
        slots = jnp.arange(CAP, dtype=jnp.int32)
        return (sel[:, :, None] & (rank[:, :, None] == slots)).astype(jnp.int32)

    serve = onehot(served // cb == me)
    blk = jnp.sum(serve * (served % cb)[:, :, None], axis=1)
    mask = jnp.sum(serve.reshape(2 * R + 1, nodes, tiles // nodes, CAP), axis=2)
    mine = rows[me]
    send = onehot((mine // cb)[None, :] == (me + offs)[:, None])
    tidx = jnp.sum(send * order[None, :, None], axis=1)
    return tidx, blk, mask.astype(F32)


def kernel(
    nb, n, scale, wscale,
    tidx, blk, msk, cells_in, embed, emix_in, cot_in, dsv_in, dproj_in, codes_in,
    hid, ngrad, wgrad,
    cells, emix, cot, dsv, dproj, codes, ls,
    buf, hbuf, hsend, hrecv, wacc, wsend, wrecv, qsend, qrecv, psend, precv, lhs, acc,
    csend, crecv, hold,
    asend, abuf,
    zs, zr, hs, hr, hps, hpr, ws, wr, qs, qr, ps, pr, zas, zar, cs, cr,
):
    me = lax.axis_index("band")
    c = lax.axis_index("chan")
    nodes = msk.shape[1]
    blkrows = cells.shape[1]
    ch = embed.shape[1]
    cb = cot.shape[0]
    krows = cb * blkrows
    cblk = cb // NCH
    hrows = NH * cblk * blkrows
    hblk = NH * cblk
    wrows = wrecv.shape[1]
    per = ch // wrows

    def rc(src, dst, ss, rs, dev):
        return pltpu.make_async_remote_copy(
            src_ref=src, dst_ref=dst, send_sem=ss, recv_sem=rs, device_id=dev, device_id_type=MESH
        )

    pos = [c, n - 1 - c]
    nxt = [lax.rem(c + 1, n), lax.rem(c + n - 1, n)]
    prv = [nxt[1], nxt[0]]

    def owner(f, d):
        return c - 1 - d if f == 0 else c + 1 + d

    def z_sends(f, d, k):
        ok = (pos[f] + 1 < n) & (pos[f] - d >= 0)
        return ok if k >= NH else ok & (pos[f] + 1 < n - 1)

    def z_copy(f, d, k):
        rows = pl.ds(k * cblk, cblk)
        src = cot.at[rows] if d == 0 else buf.at[f, d - 1, rows]
        return rc(src, buf.at[f, d, rows], zs.at[f, d, k], zr.at[f, d, k], {"chan": nxt[f]})

    def a_sends(f, d):
        return (pos[f] + 1 < n) & (pos[f] - d >= 0)

    def a_recvs(f, d):
        return pos[f] - 1 - d >= 0

    def a_copy(f, d, t):
        src = asend.at[t] if d == 0 else abuf.at[f, d - 1, t]
        return rc(src, abuf.at[f, d, t], zas.at[f, d, t], zar.at[f, d, t], {"chan": nxt[f]})

    def help_copy(f):
        return rc(dsv.at[pl.ds(0, hrows)], hbuf.at[f], hs.at[f], hr.at[f], {"chan": prv[f]})

    def part_copy(f, e):
        return rc(hsend.at[f, e], hrecv.at[f, e], hps.at[f, e], hpr.at[f, e], {"chan": nxt[f]})

    par = lax.rem(me, 2)
    sign = 1 - 2 * par
    mate = me + sign

    def turn(u):
        return u if u % 2 == 0 else -u

    def q_copy(u):
        v = turn(u)
        to = lax.rem(me + sign * u + nb, nb)
        return rc(qsend.at[u + R], qrecv.at[v + R], qs.at[u + R], qr.at[v + R], {"band": to})

    def q_from(v):
        return rc(qsend.at[v + R], qrecv.at[v + R], qs.at[v + R], qr.at[v + R], {"band": me})

    def c_copy(v):
        w = -v - 1
        return rc(csend.at[v + R], crecv.at[w + R], cs.at[v + R], cr.at[w + R], {"band": mate})

    def c_from(v):
        return rc(csend.at[v + R], crecv.at[v + R], cs.at[v + R], cr.at[v + R], {"band": mate})

    def p_copy(v, t):
        u = turn(v)
        to = lax.rem(me - sign * v + nb, nb)
        return rc(psend.at[v + R, t], precv.at[u + R, t], ps.at[v + R, t], pr.at[u + R, t], {"band": to})

    def p_from(u, t):
        return rc(psend.at[u + R, t], precv.at[u + R, t], ps.at[u + R, t], pr.at[u + R, t], {"band": me})

    def q_sends(u):
        return (me + sign * u >= 0) & (me + sign * u < nb)

    def q_recvs(v):
        return (me - sign * v >= 0) & (me - sign * v < nb)

    def p_kinds(v):
        return [par] if v in PAIRED else [0, 1]

    def w_copy(s):
        rows = pl.ds(pl.multiple_of(s * wrows, wrows), wrows)
        return rc(wsend.at[rows], wrecv.at[me], ws.at[s], wr.at[me], {"band": s})

    def w_from(s):
        rows = pl.ds(pl.multiple_of(s * wrows, wrows), wrows)
        return rc(wsend.at[rows], wrecv.at[s], ws.at[s], wr.at[s], {"band": s})

    def wdot(a, b):
        a = a.reshape(-1, ch)
        return lax.dot_general(a, b, (((0,), (0,)), ((), ())), preferred_element_type=F32)

    def w_done(own):
        rows = pl.ds(pl.multiple_of(own * ch, ch), ch)
        wsend[rows, :] = wacc[rows, :].astype(BF16)

        @pl.loop(0, per)
        def _(j):
            s = own * per + j

            @pl.when(s != me)
            def _():
                w_copy(s).start()

    def w_add(own, value, first):
        rows = pl.ds(pl.multiple_of(own * ch, ch), ch)
        if first:
            wacc[rows, :] = value
        else:
            wacc[rows, :] += value

    loads = {
        name: pltpu.make_async_copy(src, dst, ls.at[i])
        for i, (name, src, dst) in enumerate(
            (
                ("cot", cot_in, cot),
                ("codes", codes_in, codes),
                ("dsv", dsv_in, dsv),
                ("cells", cells_in, cells),
                ("emix", emix_in, emix),
                ("dproj", dproj_in, dproj),
            )
        )
    }
    for load_in in loads.values():
        load_in.start()

    barrier = pltpu.get_barrier_semaphore()

    @pl.loop(1, nb)
    def _(j):
        pl.semaphore_signal(
            barrier, inc=1, device_id={"band": lax.rem(me + j, nb)}, device_id_type=MESH
        )

    for f in range(2):
        @pl.when(pos[f] + 1 < n)
        def _():
            pl.semaphore_signal(barrier, inc=1, device_id={"chan": nxt[f]}, device_id_type=MESH)

    beside = jnp.where(c > 0, 1, 0) + jnp.where(c < n - 1, 1, 0)
    pl.semaphore_wait(barrier, nb - 1 + beside)

    loads["cot"].wait()
    loads["dsv"].wait()

    def start_own(k):
        for f in range(2):
            @pl.when(z_sends(f, 0, k))
            def _():
                z_copy(f, 0, k).start()

    for k in range(LEAD):
        start_own(k)
    for f in range(2):
        @pl.when(pos[f] == n - 1)
        def _():
            help_copy(f).start()
    for k in range(LEAD, NCH):
        start_own(k)

    loads["codes"].wait()
    for u in SEND_ORDER:
        @pl.when(q_sends(u))
        def _():
            for s in range(CAP):
                qsend[u + R, s] = (codes[tidx[u + R, s]] - 32768).astype(jnp.int16)
            q_copy(u).start()

    loads["cells"].wait()

    def serve(o, load):
        for s in range(CAP):
            word = load(s)
            cols = pl.ds(s * blkrows, blkrows)
            enc = ((word & 255) - 128).astype(F32)
            dec = (word >> 8).astype(F32)
            for m in range(nodes):
                keep = msk[o + R, m, s]
                rows = pl.ds(m * blkrows, blkrows)
                lhs[0, rows, cols] = (enc * keep).astype(BF16)
                lhs[1, rows, cols] = (dec * keep).astype(BF16)
        out = []
        for t, src in enumerate((cells, cot)):
            rhs = [src[blk[o + R, s]] for s in range(CAP)]
            out.append(jnp.dot(lhs[t], jnp.concatenate(rhs, axis=0), preferred_element_type=F32))
        return out

    def serve_own():
        own = serve(0, lambda s: codes[tidx[R, s]] - 32768)
        acc[0], acc[1] = own

    def w_own():
        w_add(c, wdot(cot[...], dsv[...]), True)
        w_done(c)

    def answer(v):
        @pl.when(q_recvs(v))
        def _():
            q_from(v).wait_recv()
            parts = serve(v, lambda s: qrecv[v + R, s].astype(jnp.int32))
            if v in PAIRED:
                hold[v + R] = jnp.where(par == 0, parts[0], parts[1])
                csend[v + R] = jnp.where(par == 0, parts[1], parts[0]).astype(BF16)
                c_copy(v).start()
            else:
                for t in range(2):
                    psend[v + R, t] = parts[t].astype(BF16)
                    p_copy(v, t).start()

    def join(v):
        @pl.when(q_recvs(v))
        def _():
            c_from(v).wait_recv()
            psend[v + R, par] = (hold[v + R] + crecv[v + R].astype(F32)).astype(BF16)
            p_copy(v, par).start()

    def aggregate():
        for v in SERVE_AT:
            u = turn(v)

            @pl.when(q_sends(u))
            def _():
                if v in PAIRED:
                    t = lax.rem(par + u + 2 * R, 2)
                    p_from(u, t).wait_recv()
                    acc[t] += precv[u + R, t].astype(F32)
                else:
                    for t in range(2):
                        p_from(u, t).wait_recv()
                        acc[t] += precv[u + R, t].astype(F32)
        for t in range(2):
            asend[t] = (acc[t] * scale).astype(BF16)
            for f in range(2):
                @pl.when(a_sends(f, 0))
                def _():
                    a_copy(f, 0, t).start()

    def take(f, p, d, k):
        @pl.when(pos[f] == p)
        def _():
            z_copy(f, d, k).wait_recv()
            if p + 1 < n - 1 or (p + 1 == n - 1 and k >= NH):
                z_copy(f, d + 1, k).start()

    def take_help(f):
        @pl.when(pos[f] == n - 2)
        def _():
            help_copy(f).wait_recv()

    def part_own(f):
        @pl.when(pos[f] == n - 2)
        def _():
            hsend[f, 0] = wdot(cot[:hblk], hbuf[f]).astype(BF16)
            part_copy(f, 0).start()

    def part_of(f, d):
        @pl.when(pos[f] == n - 2)
        def _():
            hsend[f, d + 1] = wdot(buf[f, d, :hblk], hbuf[f]).astype(BF16)
            part_copy(f, d + 1).start()

    def w_helped(f, p, d):
        @pl.when(pos[f] == p)
        def _():
            w_add(owner(f, d), wdot(buf[f, d, :hblk], dsv[:hrows]), True)

    def w_rest(f, p, d):
        @pl.when(pos[f] == p)
        def _():
            w_add(owner(f, d), wdot(buf[f, d, hblk:], dsv[hrows:]), p == n - 1)
            if p < n - 1:
                w_done(owner(f, d))

    def w_part(f, d):
        @pl.when(pos[f] == n - 1)
        def _():
            part_copy(f, d).wait_recv()
            w_add(owner(f, d), hrecv[f, d].astype(F32), False)
            w_done(owner(f, d))

    events = []

    def at(time, fn, *args):
        events.append((time, len(events), fn, args))

    def arrives(p, d, k):
        if p == n - 1:
            return k - NH + 1 if d == 0 else (d - 1) * NCH + k + 2
        if p == 1:
            return k + 1 + (NH if k >= LEAD else 0)
        return d * NCH + k + 1

    at(0.5, serve_own)
    at(1.5, w_own)
    for o, time in SERVE_AT.items():
        at(time, answer, o)
    for v, time in JOIN_AT.items():
        at(time, join, v)
    at(GATHER_AT, aggregate)
    helped_at = LEAD + NH
    for f in range(2):
        at(helped_at + 0.1, take_help, f)
        at(helped_at + 0.5, part_own, f)
        for d in range(n - 2):
            at(max(arrives(n - 2, d, NH - 1), helped_at) + 0.6, part_of, f, d)
        for p in range(1, n):
            for d in range(p):
                for k in range(NH if p == n - 1 else 0, NCH):
                    at(arrives(p, d, k), take, f, p, d, k)
                if p < n - 1:
                    at(arrives(p, d, NH - 1) + 0.7, w_helped, f, p, d)
                at(arrives(p, d, NCH - 1) + 0.4, w_rest, f, p, d)
        for d in range(n - 1):
            known = helped_at if d == 0 else max(arrives(n - 2, d - 1, NH - 1), helped_at)
            at(max(known + 2.5, arrives(n - 1, d, NCH - 1) + 0.5), w_part, f, d)
    for _, _, fn, args in sorted(events, key=lambda e: e[:2]):
        fn(*args)

    mixes = (emix, dproj)
    loads["emix"].wait()
    loads["dproj"].wait()

    def mix(t, own, value):
        rows = pl.ds(pl.multiple_of(own * ch, ch), ch)
        return jnp.dot(value, mixes[t][rows, :], preferred_element_type=F32)

    for t in range(2):
        acc[t] = mix(t, c, asend[t])

    for d in range(n - 1):
        for t in range(2):
            for f in range(2):
                @pl.when(a_recvs(f, d))
                def _():
                    a_copy(f, d, t).wait_recv()
                    if d + 1 < n - 1:
                        @pl.when(a_sends(f, d + 1))
                        def _():
                            a_copy(f, d + 1, t).start()
                    acc[t] += mix(t, owner(f, d), abuf[f, d, t])

    mixed = acc[0]
    hid[...] = (embed[...].astype(F32) + mixed / (1.0 + jnp.exp(-mixed))).astype(BF16)
    ngrad[...] = acc[1].astype(BF16)

    wgrad[...] = wacc[pl.ds(pl.multiple_of(me * wrows, wrows), wrows), :]

    @pl.loop(0, nb)
    def _(s):
        @pl.when(s != me)
        def _():
            w_from(s).wait_recv()
            wgrad[...] += wrecv[s].astype(F32)

    wgrad[...] = wgrad[...] * wscale

    for f in range(2):
        for d in range(n - 1):
            for k in range(NCH):
                @pl.when(z_sends(f, d, k))
                def _():
                    z_copy(f, d, k).wait_send()
            for t in range(2):
                @pl.when(a_sends(f, d))
                def _():
                    a_copy(f, d, t).wait_send()

            @pl.when(pos[f] == n - 2)
            def _():
                part_copy(f, d).wait_send()

        @pl.when(pos[f] == n - 1)
        def _():
            help_copy(f).wait_send()
    for u in SEND_ORDER:
        @pl.when(q_sends(u))
        def _():
            q_copy(u).wait_send()

    for v in SERVE_AT:
        @pl.when(q_recvs(v))
        def _():
            for t in p_kinds(v):
                p_copy(v, t).wait_send()
            if v in PAIRED:
                c_copy(v).wait_send()

    @pl.loop(0, nb)
    def _(s):
        @pl.when(s != me)
        def _():
            w_copy(s).wait_send()


def hand_over(hid_in, ngrad_in, wgrad_in, hid, ngrad, wgrad):
    hid[...] = hid_in[...]
    ngrad[...] = ngrad_in[...]
    wgrad[...] = wgrad_in[...]


def shards(nb, n, cells_next, node_embed, enc_mix, out_cotangent, decoded_saved, dec_proj, tile_source, tile_codes):
    me = lax.axis_index("band")
    nodes, kk, blkn, blkc = tile_codes.shape
    tiles = nodes * kk
    krows, ch = out_cotangent.shape
    cb = krows // blkc
    width = enc_mix.shape[0]
    wrows = width // nb
    scale = (3.0 / (kk * blkn)) ** 0.5 / 128.0
    wscale = float(krows * nb) ** -0.5
    tidx, blk, msk = tables_for(tile_source, me, nb, tiles, nodes, cb)
    no = 2 * R + 1
    nn = nodes * blkn
    dma = pltpu.SemaphoreType.DMA
    vm = pltpu.VMEM
    outs = pl.pallas_call(
        functools.partial(kernel, nb, n, scale, wscale),
        name="encode_and_grad",
        out_shape=(
            jax.ShapeDtypeStruct((nn, ch), BF16),
            jax.ShapeDtypeStruct((nn, ch), BF16),
            jax.ShapeDtypeStruct((wrows, ch), F32),
        ),
        in_specs=[pl.BlockSpec(memory_space=pltpu.SMEM)] * 3
        + [pl.BlockSpec(memory_space=pl.ANY), pl.BlockSpec(memory_space=vm)]
        + [pl.BlockSpec(memory_space=pl.ANY)] * 5,
        out_specs=[pl.BlockSpec(memory_space=vm)] * 3,
        scratch_shapes=[
            vm((cb, blkc, ch), BF16),
            vm((width, ch), BF16),
            vm((cb, blkc, ch), BF16),
            vm((krows, ch), BF16),
            vm((width, ch), BF16),
            vm((tiles, blkn, blkc), jnp.int32),
            dma((6,)),
            vm((2, n - 1, cb, blkc, ch), BF16),
            vm((2, krows * NH // NCH, ch), BF16),
            vm((2, n - 1, ch, ch), BF16),
            vm((2, n - 1, ch, ch), BF16),
            vm((width, ch), F32),
            vm((width, ch), BF16),
            vm((nb, wrows, ch), BF16),
            vm((no, CAP, blkn, blkc), jnp.int16),
            vm((no, CAP, blkn, blkc), jnp.int16),
            vm((no, 2, nn, ch), BF16),
            vm((no, 2, nn, ch), BF16),
            vm((2, nn, CAP * blkc), BF16),
            vm((2, nn, ch), F32),
            vm((no, nn, ch), BF16),
            vm((no, nn, ch), BF16),
            vm((no, nn, ch), F32),
            vm((2, nn, ch), BF16),
            vm((2, n - 1, 2, nn, ch), BF16),
            dma((2, n - 1, NCH)),
            dma((2, n - 1, NCH)),
            dma((2,)),
            dma((2,)),
            dma((2, n - 1)),
            dma((2, n - 1)),
            dma((nb,)),
            dma((nb,)),
            dma((no,)),
            dma((no,)),
            dma((no, 2)),
            dma((no, 2)),
            dma((2, n - 1, 2)),
            dma((2, n - 1, 2)),
            dma((no,)),
            dma((no,)),
        ],
        compiler_params=pltpu.CompilerParams(
            collective_id=0, has_side_effects=True, vmem_limit_bytes=56 * 1024 * 1024
        ),
    )(
        tidx, blk, msk,
        cells_next.reshape(cb, blkc, ch), node_embed, enc_mix,
        out_cotangent.reshape(cb, blkc, ch), decoded_saved, dec_proj,
        tile_codes.reshape(tiles, blkn, blkc),
    )
    return pl.pallas_call(
        hand_over,
        name="hand_over",
        out_shape=tuple(jax.ShapeDtypeStruct(x.shape, x.dtype) for x in outs),
        in_specs=[pl.BlockSpec(memory_space=vm)] * 3,
        out_specs=[pl.BlockSpec(memory_space=vm)] * 3,
    )(*outs)


def solution(mesh):
    nb, n = mesh.shape["band"], mesh.shape["chan"]
    in_specs = (
        P("band", "chan"),
        P("band", "chan"),
        P(None, "chan"),
        P("band", "chan"),
        P("band", "chan"),
        P(None, "chan"),
        P(),
        P("band", None, None, None),
    )
    out_specs = (P("band", "chan"), P("band", "chan"), P("band", "chan"))
    return jax.shard_map(
        functools.partial(shards, nb, n),
        mesh=mesh,
        in_specs=in_specs,
        out_specs=out_specs,
        check_vma=False,
    )
```

```python
import functools

import jax
import jax.numpy as jnp
from jax import lax
from jax.experimental import pallas as pl
from jax.experimental.pallas import tpu as pltpu
from jax.sharding import PartitionSpec as P

R = 3
CAP = 8
SEND_ORDER = [3, 2, -2, -1, -3, 1]
MATE = -1
PAIRED = {v for v in range(-R, R + 1) if v not in (0, MATE) and -v - 1 not in (0, MATE) and -R <= -v - 1 <= R}
SERVE_AT = {-3: 2.6, 2: 4.6, -2: 6.6, 1: 7.6, 3: 7.7, -1: 7.8}
JOIN_AT = {-3: 4.7, 2: 4.8, -2: 7.9, 1: 8.0}
GATHER_AT = 10.6
NCH = 8
NH = 6
LEAD = NCH // 2
AP = 2
WSUM = 2
MESH = pl.DeviceIdType.MESH
F32 = jnp.float32
BF16 = jnp.bfloat16


def kernel(
    nb, n, scale, wscale,
    src_of, cells_in, embed_in, emix_in, cot_in, dsv_in, dproj_in, codes_in,
    hid_out, ngrad_out, wgrad_out,
    hid, ngrad, wgrad, outs,
    cells, embed, emix, cot, dsv, dproj, codes, ls,
    buf, hbuf, hsend, hrecv, wacc, wsend, wrecv, qsend, qrecv, psend, precv, lhs, acc,
    csend, crecv, hold,
    asend, abuf,
    zs, zr, hs, hr, hps, hpr, ws, wr, qs, qr, ps, pr, zas, zar, cs, cr,
):
    me = lax.axis_index("band")
    c = lax.axis_index("chan")
    kk = src_of.shape[1]
    nodes = codes.shape[0] // kk
    blkrows = cells.shape[1]
    ch = embed.shape[1]
    cb = cot.shape[0]
    krows = cb * blkrows
    cblk = cb // NCH
    hrows = NH * cblk * blkrows
    hblk = NH * cblk
    wrows = wrecv.shape[1]
    per = ch // wrows

    def rc(src, dst, ss, rs, dev):
        return pltpu.make_async_remote_copy(
            src_ref=src, dst_ref=dst, send_sem=ss, recv_sem=rs, device_id=dev, device_id_type=MESH
        )

    pos = [c, n - 1 - c]
    nxt = [lax.rem(c + 1, n), lax.rem(c + n - 1, n)]
    prv = [nxt[1], nxt[0]]

    def owner(f, d):
        return c - 1 - d if f == 0 else c + 1 + d

    def z_sends(f, d, k):
        ok = (pos[f] + 1 < n) & (pos[f] - d >= 0)
        return ok if k >= NH else ok & (pos[f] + 1 < n - 1)

    def z_copy(f, d, k):
        rows = pl.ds(k * cblk, cblk)
        src = cot.at[rows] if d == 0 else buf.at[f, d - 1, rows]
        return rc(src, buf.at[f, d, rows], zs.at[f, d, k], zr.at[f, d, k], {"chan": nxt[f]})

    def a_sends(f, d):
        return (pos[f] + 1 < n) & (pos[f] - d >= 0)

    arows = embed.shape[0] // AP

    def a_copy(f, d, t, h):
        rows = pl.ds(h * arows, arows)
        src = asend.at[t, rows] if d == 0 else abuf.at[f, d - 1, t, rows]
        return rc(src, abuf.at[f, d, t, rows], zas.at[f, d, t, h], zar.at[f, d, t, h], {"chan": nxt[f]})

    def help_copy(f):
        return rc(dsv.at[pl.ds(0, hrows)], hbuf.at[f], hs.at[f], hr.at[f], {"chan": prv[f]})

    def part_copy(f, e):
        return rc(hsend.at[f, e], hrecv.at[f, e], hps.at[f, e], hpr.at[f, e], {"chan": nxt[f]})

    par = lax.rem(me, 2)
    sign = 1 - 2 * par
    mate = me + sign

    def turn(u):
        return u if u % 2 == 0 else -u

    def picks(band, wanted):
        low = wanted * cb
        bits = (max(cb, kk) - 1).bit_length()
        one = jnp.int32(1)
        zero = jnp.int32(0)
        seen, block, place, part = zero, zero, zero, zero
        unit, flag = one, one
        for m in range(nodes):
            for k in range(kk):
                off = src_of[band * nodes + m, k] - low
                hit = (off >= 0) & (off < cb)
                block += jnp.where(hit, off * unit, 0)
                place += jnp.where(hit, k * unit, 0)
                part += jnp.where(hit, m * flag, 0)
                seen += jnp.where(hit, 1, 0)
                unit = jnp.where(hit, unit * 2**bits, unit)
                flag = jnp.where(hit, flag * nodes, flag)

        def field(word, s, size):
            return (word >> (size * s)) & (2**size - 1)

        mbits = (nodes - 1).bit_length()
        slots = []
        for s in range(CAP):
            m = field(part, s, mbits)
            keeps = [jnp.where((m == i) & (s < seen), 1.0, 0.0) for i in range(nodes)]
            slots.append((m * kk + field(place, s, bits), field(block, s, bits), keeps))
        return slots

    def q_copy(u):
        v = turn(u)
        to = lax.rem(me + sign * u + nb, nb)
        return rc(qsend.at[u + R], qrecv.at[v + R], qs.at[u + R], qr.at[v + R], {"band": to})

    def q_from(v):
        return rc(qsend.at[v + R], qrecv.at[v + R], qs.at[v + R], qr.at[v + R], {"band": me})

    def c_copy(v):
        w = -v - 1
        return rc(csend.at[v + R], crecv.at[w + R], cs.at[v + R], cr.at[w + R], {"band": mate})

    def c_from(v):
        return rc(csend.at[v + R], crecv.at[v + R], cs.at[v + R], cr.at[v + R], {"band": mate})

    def p_copy(v, t):
        u = turn(v)
        to = lax.rem(me - sign * v + nb, nb)
        return rc(psend.at[v + R, t], precv.at[u + R, t], ps.at[v + R, t], pr.at[u + R, t], {"band": to})

    def p_from(u, t):
        return rc(psend.at[u + R, t], precv.at[u + R, t], ps.at[u + R, t], pr.at[u + R, t], {"band": me})

    def q_sends(u):
        return (me + sign * u >= 0) & (me + sign * u < nb)

    def q_recvs(v):
        return (me - sign * v >= 0) & (me - sign * v < nb)

    def p_kinds(v):
        return [par] if v in PAIRED else [0, 1]

    def w_copy(s):
        rows = pl.ds(pl.multiple_of(s * wrows, wrows), wrows)
        return rc(wsend.at[rows], wrecv.at[me], ws.at[s], wr.at[me], {"band": s})

    def w_from(s):
        rows = pl.ds(pl.multiple_of(s * wrows, wrows), wrows)
        return rc(wsend.at[rows], wrecv.at[s], ws.at[s], wr.at[s], {"band": s})

    def wdot(a, b):
        a = a.reshape(-1, ch)
        return lax.dot_general(a, b, (((0,), (0,)), ((), ())), preferred_element_type=F32)

    def w_done(own):
        rows = pl.ds(pl.multiple_of(own * ch, ch), ch)
        wsend[rows, :] = wacc[rows, :].astype(BF16)

        @pl.loop(0, per)
        def _(j):
            s = own * per + j

            @pl.when(s != me)
            def _():
                w_copy(s).start()

    def w_add(own, value, first):
        rows = pl.ds(pl.multiple_of(own * ch, ch), ch)
        if first:
            wacc[rows, :] = value
        else:
            wacc[rows, :] += value

    loads = {
        name: pltpu.make_async_copy(src, dst, ls.at[i])
        for i, (name, src, dst) in enumerate(
            (
                ("cot", cot_in, cot),
                ("codes", codes_in, codes),
                ("dsv", dsv_in, dsv),
                ("cells", cells_in, cells),
                ("emix", emix_in, emix),
                ("dproj", dproj_in, dproj),
                ("embed", embed_in, embed),
            )
        )
    }
    for load_in in loads.values():
        load_in.start()

    barrier = pltpu.get_barrier_semaphore()

    @pl.loop(1, nb)
    def _(j):
        pl.semaphore_signal(
            barrier, inc=1, device_id={"band": lax.rem(me + j, nb)}, device_id_type=MESH
        )

    for f in range(2):
        @pl.when(pos[f] + 1 < n)
        def _():
            pl.semaphore_signal(barrier, inc=1, device_id={"chan": nxt[f]}, device_id_type=MESH)

    beside = jnp.where(c > 0, 1, 0) + jnp.where(c < n - 1, 1, 0)
    pl.semaphore_wait(barrier, nb - 1 + beside)

    loads["cot"].wait()
    loads["dsv"].wait()

    def start_own(k):
        for f in range(2):
            @pl.when(z_sends(f, 0, k))
            def _():
                z_copy(f, 0, k).start()

    for k in range(LEAD):
        start_own(k)
    for f in range(2):
        @pl.when(pos[f] == n - 1)
        def _():
            help_copy(f).start()
    for k in range(LEAD, NCH):
        start_own(k)

    loads["codes"].wait()
    for u in SEND_ORDER:
        @pl.when(q_sends(u))
        def _():
            for s, (tile, _, _) in enumerate(picks(me, me + sign * u)):
                qsend[u + R, s] = (codes[tile] - 32768).astype(jnp.int16)
            q_copy(u).start()

    loads["cells"].wait()

    def serve(slots, load):
        for s, (tile, _, keeps) in enumerate(slots):
            word = load(s, tile)
            cols = pl.ds(s * blkrows, blkrows)
            enc = ((word & 255) - 128).astype(F32)
            dec = (word >> 8).astype(F32)
            for m in range(nodes):
                keep = keeps[m]
                rows = pl.ds(m * blkrows, blkrows)
                lhs[0, rows, cols] = (enc * keep).astype(BF16)
                lhs[1, rows, cols] = (dec * keep).astype(BF16)
        out = []
        for t, src in enumerate((cells, cot)):
            rhs = [src[block] for _, block, _ in slots]
            out.append(jnp.dot(lhs[t], jnp.concatenate(rhs, axis=0), preferred_element_type=F32))
        return out

    def serve_own():
        own = serve(picks(me, me), lambda s, tile: codes[tile] - 32768)
        acc[0], acc[1] = own

    def w_own():
        w_add(c, wdot(cot[...], dsv[...]), True)
        w_done(c)

    def answer(v):
        @pl.when(q_recvs(v))
        def _():
            slots = picks(me - sign * v, me)
            q_from(v).wait_recv()
            parts = serve(slots, lambda s, tile: qrecv[v + R, s].astype(jnp.int32))
            if v in PAIRED:
                hold[v + R] = jnp.where(par == 0, parts[0], parts[1])
                csend[v + R] = jnp.where(par == 0, parts[1], parts[0]).astype(BF16)
                c_copy(v).start()
            else:
                for t in range(2):
                    psend[v + R, t] = parts[t].astype(BF16)
                    p_copy(v, t).start()

    def join(v):
        @pl.when(q_recvs(v))
        def _():
            c_from(v).wait_recv()
            psend[v + R, par] = (hold[v + R] + crecv[v + R].astype(F32)).astype(BF16)
            p_copy(v, par).start()

    def aggregate():
        for v in SERVE_AT:
            u = turn(v)

            @pl.when(q_sends(u))
            def _():
                if v in PAIRED:
                    t = lax.rem(par + u + 2 * R, 2)
                    p_from(u, t).wait_recv()
                    acc[t] += precv[u + R, t].astype(F32)
                else:
                    for t in range(2):
                        p_from(u, t).wait_recv()
                        acc[t] += precv[u + R, t].astype(F32)
        for t in range(2):
            asend[t] = (acc[t] * scale).astype(BF16)
        for f in range(2):
            @pl.when((pos[f] == 0) | (pos[f] == n - 2))
            def _():
                a_start(f)

    def a_start(f):
        for t in range(2):
            for h in range(AP):
                a_copy(f, 0, t, h).start()

    def a_own(f, p):
        @pl.when(pos[f] == p)
        def _():
            a_start(f)

    mixes = (emix, dproj)

    def mix(t, own, value):
        rows = pl.ds(pl.multiple_of(own * ch, ch), ch)
        return jnp.dot(value, mixes[t][rows, :], preferred_element_type=F32)

    def mix_own():
        loads["embed"].wait()
        loads["emix"].wait()
        loads["dproj"].wait()
        for t in range(2):
            acc[t] = mix(t, c, asend[t])

    def a_take(f, p, d, t, h):
        @pl.when(pos[f] == p)
        def _():
            a_copy(f, d, t, h).wait_recv()
            if p + 1 < n:
                a_copy(f, d + 1, t, h).start()
            rows = pl.ds(h * arows, arows)
            acc[t, rows, :] += mix(t, owner(f, d), abuf[f, d, t, rows, :])

    def finish(t):
        if t == 0:
            mixed = acc[0]
            hid[...] = (embed[...].astype(F32) + mixed / (1.0 + jnp.exp(-mixed))).astype(BF16)
            stores[0].start()
        else:
            ngrad[...] = acc[1].astype(BF16)
            stores[1].start()

    stores = [
        pltpu.make_async_copy(src, dst, outs.at[i])
        for i, (src, dst) in enumerate(((hid, hid_out), (ngrad, ngrad_out), (wgrad, wgrad_out)))
    ]

    def take(f, p, d, k):
        @pl.when(pos[f] == p)
        def _():
            z_copy(f, d, k).wait_recv()
            if p + 1 < n - 1 or (p + 1 == n - 1 and k >= NH):
                z_copy(f, d + 1, k).start()

    def take_help(f):
        @pl.when(pos[f] == n - 2)
        def _():
            help_copy(f).wait_recv()

    def part_own(f):
        @pl.when(pos[f] == n - 2)
        def _():
            hsend[f, 0] = wdot(cot[:hblk], hbuf[f]).astype(BF16)
            part_copy(f, 0).start()

    def part_of(f, d):
        @pl.when(pos[f] == n - 2)
        def _():
            hsend[f, d + 1] = wdot(buf[f, d, :hblk], hbuf[f]).astype(BF16)
            part_copy(f, d + 1).start()

    def w_helped(f, p, d):
        @pl.when(pos[f] == p)
        def _():
            w_add(owner(f, d), wdot(buf[f, d, :hblk], dsv[:hrows]), True)

    def w_rest(f, p, d):
        @pl.when(pos[f] == p)
        def _():
            w_add(owner(f, d), wdot(buf[f, d, hblk:], dsv[hrows:]), p == n - 1)
            if p < n - 1:
                w_done(owner(f, d))

    def w_part(f, d):
        @pl.when(pos[f] == n - 1)
        def _():
            part_copy(f, d).wait_recv()
            w_add(owner(f, d), hrecv[f, d].astype(F32), False)
            w_done(owner(f, d))

    def w_sum():
        total = wacc[pl.ds(pl.multiple_of(me * wrows, wrows), wrows), :]
        wgrad[...] = total

        @pl.loop(0, nb)
        def _(s):
            @pl.when(s != me)
            def _():
                w_from(s).wait_recv()
                wgrad[...] += wrecv[s].astype(F32)

        wgrad[...] = wgrad[...] * wscale
        stores[2].start()

    def drain_a():
        for f in range(2):
            for d in range(n - 1):
                @pl.when(a_sends(f, d))
                def _():
                    for t in range(2):
                        for h in range(AP):
                            a_copy(f, d, t, h).wait_send()

    def drain_w():
        @pl.loop(0, nb)
        def _(s):
            @pl.when(s != me)
            def _():
                w_copy(s).wait_send()

    def drain_stores():
        for store in stores:
            store.wait()

    def drain():
        for f in range(2):
            for d in range(n - 1):
                for k in range(NCH):
                    @pl.when(z_sends(f, d, k))
                    def _():
                        z_copy(f, d, k).wait_send()

                @pl.when(pos[f] == n - 2)
                def _():
                    part_copy(f, d).wait_send()

            @pl.when(pos[f] == n - 1)
            def _():
                help_copy(f).wait_send()
        for u in SEND_ORDER:
            @pl.when(q_sends(u))
            def _():
                q_copy(u).wait_send()

        for v in SERVE_AT:
            @pl.when(q_recvs(v))
            def _():
                for t in p_kinds(v):
                    p_copy(v, t).wait_send()
                if v in PAIRED:
                    c_copy(v).wait_send()

    events = []

    def at(time, fn, *args):
        events.append((time, len(events), fn, args))

    def arrives(p, d, k):
        if p == n - 1:
            return k - NH + 1 if d == 0 else (d - 1) * NCH + k + 2
        if p == 1:
            return k + 1 + (NH if k >= LEAD else 0)
        return d * NCH + k + 1

    at(0.5, serve_own)
    at(1.5, w_own)
    for o, time in SERVE_AT.items():
        at(time, answer, o)
    for v, time in JOIN_AT.items():
        at(time, join, v)
    at(GATHER_AT, aggregate)
    at(GATHER_AT + 0.3, mix_own)
    last = 2 * NCH + 2 * n

    def a_arrives(p, d):
        if p == n - 1:
            return GATHER_AT + 2.5 if d == 0 else a_arrives(p - 1, d - 1) + 1.5
        return 2 * NCH + 0.5 + 2 * (d + 1)

    helped_at = LEAD + NH
    for f in range(2):
        at(helped_at + 0.1, take_help, f)
        at(helped_at + 0.5, part_own, f)
        for d in range(n - 2):
            at(max(arrives(n - 2, d, NH - 1), helped_at) + 0.6, part_of, f, d)
        for p in range(1, n):
            for d in range(p):
                for k in range(NH if p == n - 1 else 0, NCH):
                    at(arrives(p, d, k), take, f, p, d, k)
                if p < n - 1:
                    at(arrives(p, d, NH - 1) + 0.7, w_helped, f, p, d)
                at(arrives(p, d, NCH - 1) + 0.4, w_rest, f, p, d)
        for d in range(n - 1):
            known = helped_at if d == 0 else max(arrives(n - 2, d - 1, NH - 1), helped_at)
            at(max(known + 2.5, arrives(n - 1, d, NCH - 1) + 0.5), w_part, f, d)
    for f in range(2):
        for p in range(1, n):
            if p + 1 < n - 1:
                at(max(GATHER_AT, arrives(p, p - 1, NCH - 1)) + 0.35, a_own, f, p)
            for d in range(p):
                for t in range(2):
                    for h in range(AP):
                        when = a_arrives(p, d) + (t * AP + h) / AP
                        at(when if p < n - 1 or d < n - 2 else last + t + h / AP, a_take, f, p, d, t, h)
    at(last + 0.9, finish, 0)
    at(last + WSUM, w_sum)
    at(last + 1.9, finish, 1)
    for i, fn in enumerate((drain, drain_w, drain_a, drain_stores)):
        at(last + 3 + i, fn)
    for _, _, fn, args in sorted(events, key=lambda e: e[:2]):
        fn(*args)


def hand_over(hid_in, ngrad_in, wgrad_in, hid, ngrad, wgrad):
    hid[...] = hid_in[...]
    ngrad[...] = ngrad_in[...]
    wgrad[...] = wgrad_in[...]


def shards(nb, n, cells_next, node_embed, enc_mix, out_cotangent, decoded_saved, dec_proj, tile_source, tile_codes):
    nodes, kk, blkn, blkc = tile_codes.shape
    tiles = nodes * kk
    krows, ch = out_cotangent.shape
    cb = krows // blkc
    width = enc_mix.shape[0]
    wrows = width // nb
    scale = (3.0 / (kk * blkn)) ** 0.5 / 128.0
    wscale = float(krows * nb) ** -0.5
    no = 2 * R + 1
    nn = nodes * blkn
    dma = pltpu.SemaphoreType.DMA
    vm = pltpu.VMEM
    outs = pl.pallas_call(
        functools.partial(kernel, nb, n, scale, wscale),
        name="encode_and_grad",
        out_shape=(
            jax.ShapeDtypeStruct((nn, ch), BF16),
            jax.ShapeDtypeStruct((nn, ch), BF16),
            jax.ShapeDtypeStruct((wrows, ch), F32),
        ),
        in_specs=[pl.BlockSpec(memory_space=pltpu.SMEM)] + [pl.BlockSpec(memory_space=pl.ANY)] * 7,
        out_specs=[pl.BlockSpec(memory_space=pl.ANY)] * 3,
        scratch_shapes=[
            vm((nn, ch), BF16),
            vm((nn, ch), BF16),
            vm((wrows, ch), F32),
            dma((3,)),
            vm((cb, blkc, ch), BF16),
            vm((nn, ch), BF16),
            vm((width, ch), BF16),
            vm((cb, blkc, ch), BF16),
            vm((krows, ch), BF16),
            vm((width, ch), BF16),
            vm((tiles, blkn, blkc), jnp.int32),
            dma((7,)),
            vm((2, n - 1, cb, blkc, ch), BF16),
            vm((2, krows * NH // NCH, ch), BF16),
            vm((2, n - 1, ch, ch), BF16),
            vm((2, n - 1, ch, ch), BF16),
            vm((width, ch), F32),
            vm((width, ch), BF16),
            vm((nb, wrows, ch), BF16),
            vm((no, CAP, blkn, blkc), jnp.int16),
            vm((no, CAP, blkn, blkc), jnp.int16),
            vm((no, 2, nn, ch), BF16),
            vm((no, 2, nn, ch), BF16),
            vm((2, nn, CAP * blkc), BF16),
            vm((2, nn, ch), F32),
            vm((no, nn, ch), BF16),
            vm((no, nn, ch), BF16),
            vm((no, nn, ch), F32),
            vm((2, nn, ch), BF16),
            vm((2, n - 1, 2, nn, ch), BF16),
            dma((2, n - 1, NCH)),
            dma((2, n - 1, NCH)),
            dma((2,)),
            dma((2,)),
            dma((2, n - 1)),
            dma((2, n - 1)),
            dma((nb,)),
            dma((nb,)),
            dma((no,)),
            dma((no,)),
            dma((no, 2)),
            dma((no, 2)),
            dma((2, n - 1, 2, AP)),
            dma((2, n - 1, 2, AP)),
            dma((no,)),
            dma((no,)),
        ],
        compiler_params=pltpu.CompilerParams(
            collective_id=0, has_side_effects=True, vmem_limit_bytes=56 * 1024 * 1024
        ),
    )(
        tile_source,
        cells_next.reshape(cb, blkc, ch), node_embed, enc_mix,
        out_cotangent.reshape(cb, blkc, ch), decoded_saved, dec_proj,
        tile_codes.reshape(tiles, blkn, blkc),
    )
    return pl.pallas_call(
        hand_over,
        name="hand_over",
        out_shape=tuple(jax.ShapeDtypeStruct(x.shape, x.dtype) for x in outs),
        in_specs=[pl.BlockSpec(memory_space=vm)] * 3,
        out_specs=[pl.BlockSpec(memory_space=vm)] * 3,
    )(*outs)


def solution(mesh):
    nb, n = mesh.shape["band"], mesh.shape["chan"]
    in_specs = (
        P("band", "chan"),
        P("band", "chan"),
        P(None, "chan"),
        P("band", "chan"),
        P("band", "chan"),
        P(None, "chan"),
        P(),
        P("band", None, None, None),
    )
    out_specs = (P("band", "chan"), P("band", "chan"), P("band", "chan"))
    return jax.shard_map(
        functools.partial(shards, nb, n),
        mesh=mesh,
        in_specs=in_specs,
        out_specs=out_specs,
        check_vma=False,
    )
```

```python
import functools

import jax
import jax.numpy as jnp
from jax import lax
from jax.experimental import pallas as pl
from jax.experimental.pallas import tpu as pltpu
from jax.sharding import PartitionSpec as P

R = 3
CAP = 8
SEND_ORDER = [3, 2, -2, -1, -3, 1]
MATE = -1
PAIRED = {v for v in range(-R, R + 1) if v not in (0, MATE) and -v - 1 not in (0, MATE) and -R <= -v - 1 <= R}
SERVE_AT = {-3: 2.6, 2: 4.6, -2: 6.6, 1: 7.6, 3: 7.7, -1: 7.8}
JOIN_AT = {-3: 4.7, 2: 4.8, -2: 7.9, 1: 8.0}
GATHER_AT = 12.3
NCH = 8
NH = 6
LEAD = 4
AP = 2
WSUM = 2
MESH = pl.DeviceIdType.MESH
F32 = jnp.float32
BF16 = jnp.bfloat16


def kernel(
    nb, n, scale, wscale,
    src_of, cells_in, embed_in, emix_in, cot_in, dsv_in, dproj_in, codes_in,
    hid_out, ngrad_out, wgrad_out,
    hid, ngrad, wgrad, outs,
    cells, embed, emix, cot, dsv, dproj, codes, ls,
    buf, hbuf, hsend, hrecv, wacc, wsend, wrecv, qsend, qrecv, psend, precv, lhs, acc,
    csend, crecv, hold,
    asend, abuf,
    zs, zr, hs, hr, hps, hpr, ws, wr, qs, qr, ps, pr, zas, zar, cs, cr,
):
    me = lax.axis_index("band")
    c = lax.axis_index("chan")
    kk = src_of.shape[1]
    nodes = codes.shape[0] // kk
    blkrows = cells.shape[1]
    ch = embed.shape[1]
    cb = cot.shape[0]
    krows = cb * blkrows
    cblk = cb // NCH
    hrows = NH * cblk * blkrows
    hblk = NH * cblk
    wrows = wrecv.shape[1]
    per = ch // wrows

    def rc(src, dst, ss, rs, dev):
        return pltpu.make_async_remote_copy(
            src_ref=src, dst_ref=dst, send_sem=ss, recv_sem=rs, device_id=dev, device_id_type=MESH
        )

    pos = [c, n - 1 - c]
    nxt = [lax.rem(c + 1, n), lax.rem(c + n - 1, n)]
    prv = [nxt[1], nxt[0]]

    def owner(f, d):
        return c - 1 - d if f == 0 else c + 1 + d

    def z_sends(f, d, k):
        ok = (pos[f] + 1 < n) & (pos[f] - d >= 0)
        return ok if k >= NH else ok & (pos[f] + 1 < n - 1)

    def slot_at(f, d, ahead):
        return d if f == 0 else d + c - ahead

    def z_copy(f, d, k):
        rows = pl.ds(k * cblk, cblk)
        src = cot.at[rows] if d == 0 else buf.at[f, d - 1, rows]
        return rc(src, buf.at[f, d, rows], zs.at[f, d], zr.at[slot_at(f, d, 1), k], {"chan": nxt[f]})

    def z_from(f, d, k):
        rows = pl.ds(k * cblk, cblk)
        dst = buf.at[f, d, rows]
        return rc(dst, dst, zs.at[f, d], zr.at[slot_at(f, d, 0), k], {"chan": nxt[f]})

    def z_sent(f, d, first):
        rows = pl.ds(first * cblk, cb - first * cblk)
        dst = buf.at[f, d, rows]
        return rc(dst, dst, zs.at[f, d], zr.at[0, 0], {"chan": nxt[f]})

    def a_sends(f, d):
        return (pos[f] + 1 < n) & (pos[f] - d >= 0)

    arows = embed.shape[0] // AP

    def a_copy(f, d, t, h):
        rows = pl.ds(h * arows, arows)
        src = asend.at[t, rows] if d == 0 else abuf.at[f, d - 1, t, rows]
        return rc(src, abuf.at[f, d, t, rows], zas.at[f, d], zar.at[slot_at(f, d, 1), t, h], {"chan": nxt[f]})

    def a_from(f, d, t, h):
        dst = abuf.at[f, d, t, pl.ds(h * arows, arows)]
        return rc(dst, dst, zas.at[f, d], zar.at[slot_at(f, d, 0), t, h], {"chan": nxt[f]})

    def a_sent(f, d):
        dst = abuf.at[f, d]
        return rc(dst, dst, zas.at[f, d], zar.at[0, 0, 0], {"chan": nxt[f]})

    def help_copy(f):
        return rc(dsv.at[pl.ds(0, hrows)], hbuf.at[f], hs.at[f], hr.at[f], {"chan": prv[f]})

    def part_copy(f, e):
        return rc(hsend.at[f, e], hrecv.at[f, e], hps.at[f, e], hpr.at[f, e], {"chan": nxt[f]})

    par = lax.rem(me, 2)
    sign = 1 - 2 * par
    mate = me + sign

    def turn(u):
        return u if u % 2 == 0 else -u

    def picks(band, wanted):
        low = wanted * cb
        bits = (max(cb, kk) - 1).bit_length()
        one = jnp.int32(1)
        zero = jnp.int32(0)
        seen, block, place, part = zero, zero, zero, zero
        unit, flag = one, one
        for m in range(nodes):
            for k in range(kk):
                off = src_of[band * nodes + m, k] - low
                hit = (off >= 0) & (off < cb)
                block += jnp.where(hit, off * unit, 0)
                place += jnp.where(hit, k * unit, 0)
                part += jnp.where(hit, m * flag, 0)
                seen += jnp.where(hit, 1, 0)
                unit = jnp.where(hit, unit * 2**bits, unit)
                flag = jnp.where(hit, flag * nodes, flag)

        def field(word, s, size):
            return (word >> (size * s)) & (2**size - 1)

        mbits = (nodes - 1).bit_length()
        slots = []
        for s in range(CAP):
            m = field(part, s, mbits)
            keeps = [jnp.where((m == i) & (s < seen), 1.0, 0.0) for i in range(nodes)]
            slots.append((m * kk + field(place, s, bits), field(block, s, bits), keeps))
        return slots

    def q_copy(u):
        v = turn(u)
        to = lax.rem(me + sign * u + nb, nb)
        return rc(qsend.at[u + R], qrecv.at[v + R], qs.at[u + R], qr.at[v + R], {"band": to})

    def q_from(v):
        return rc(qsend.at[v + R], qrecv.at[v + R], qs.at[v + R], qr.at[v + R], {"band": me})

    def c_copy(v):
        w = -v - 1
        return rc(csend.at[v + R], crecv.at[w + R], cs.at[v + R], cr.at[w + R], {"band": mate})

    def c_from(v):
        return rc(csend.at[v + R], crecv.at[v + R], cs.at[v + R], cr.at[v + R], {"band": mate})

    def p_copy(v, t):
        u = turn(v)
        to = lax.rem(me - sign * v + nb, nb)
        return rc(psend.at[v + R, t], precv.at[u + R, t], ps.at[v + R], pr.at[u + R, t], {"band": to})

    def p_sent(v):
        src = psend.at[v + R, 0] if v in PAIRED else psend.at[v + R]
        return rc(src, src, ps.at[v + R], ps.at[v + R], {"band": me})

    def p_from(u, t):
        return rc(psend.at[u + R, t], precv.at[u + R, t], ps.at[u + R], pr.at[u + R, t], {"band": me})

    def q_sends(u):
        return (me + sign * u >= 0) & (me + sign * u < nb)

    def q_recvs(v):
        return (me - sign * v >= 0) & (me - sign * v < nb)

    def w_copy(s):
        rows = pl.ds(pl.multiple_of(s * wrows, wrows), wrows)
        return rc(wsend.at[rows], wrecv.at[me], ws.at[0], wr.at[0], {"band": s})

    def w_all():
        rows = wsend.at[pl.ds(0, (nb - 1) * wrows)]
        return rc(rows, rows, ws.at[0], ws.at[0], {"band": me})

    def w_got():
        blocks = wrecv.at[pl.ds(0, nb - 1)]
        return rc(blocks, blocks, wr.at[0], wr.at[0], {"band": me})

    def wdot(a, b):
        a = a.reshape(-1, ch)
        return lax.dot_general(a, b, (((0,), (0,)), ((), ())), preferred_element_type=F32)

    def w_done(own):
        rows = pl.ds(pl.multiple_of(own * ch, ch), ch)
        wsend[rows, :] = wacc[rows, :].astype(BF16)

        @pl.loop(0, per)
        def _(j):
            s = own * per + j

            @pl.when(s != me)
            def _():
                w_copy(s).start()

    def w_add(own, value, first):
        rows = pl.ds(pl.multiple_of(own * ch, ch), ch)
        if first:
            wacc[rows, :] = value
        else:
            wacc[rows, :] += value

    loads = {
        name: pltpu.make_async_copy(src, dst, ls.at[i])
        for i, (name, src, dst) in enumerate(
            (
                ("cot", cot_in, cot),
                ("codes", codes_in, codes),
                ("dsv", dsv_in, dsv),
                ("cells", cells_in, cells),
                ("emix", emix_in, emix),
                ("dproj", dproj_in, dproj),
                ("embed", embed_in, embed),
            )
        )
    }
    for load_in in loads.values():
        load_in.start()

    barrier = pltpu.get_barrier_semaphore()

    @pl.loop(1, nb)
    def _(j):
        pl.semaphore_signal(
            barrier, inc=1, device_id={"band": lax.rem(me + j, nb)}, device_id_type=MESH
        )

    for f in range(2):
        @pl.when(pos[f] + 1 < n)
        def _():
            pl.semaphore_signal(barrier, inc=1, device_id={"chan": nxt[f]}, device_id_type=MESH)

    beside = jnp.where(c > 0, 1, 0) + jnp.where(c < n - 1, 1, 0)
    pl.semaphore_wait(barrier, nb - 1 + beside)

    loads["cot"].wait()
    loads["dsv"].wait()

    def start_own(k):
        for f in range(2):
            @pl.when(z_sends(f, 0, k))
            def _():
                z_copy(f, 0, k).start()

    for k in range(LEAD):
        start_own(k)
    for f in range(2):
        @pl.when(pos[f] == n - 1)
        def _():
            help_copy(f).start()
    for k in range(LEAD, NCH):
        start_own(k)

    loads["codes"].wait()
    for u in SEND_ORDER:
        @pl.when(q_sends(u))
        def _():
            for s, (tile, _, _) in enumerate(picks(me, me + sign * u)):
                qsend[u + R, s] = (codes[tile] - 32768).astype(jnp.int16)
            q_copy(u).start()

    loads["cells"].wait()

    def serve(slots, load):
        for s, (tile, _, keeps) in enumerate(slots):
            word = load(s, tile)
            cols = pl.ds(s * blkrows, blkrows)
            enc = ((word & 255) - 128).astype(F32)
            dec = (word >> 8).astype(F32)
            for m in range(nodes):
                keep = keeps[m]
                rows = pl.ds(m * blkrows, blkrows)
                lhs[0, rows, cols] = (enc * keep).astype(BF16)
                lhs[1, rows, cols] = (dec * keep).astype(BF16)
        out = []
        for t, src in enumerate((cells, cot)):
            rhs = [src[block] for _, block, _ in slots]
            out.append(jnp.dot(lhs[t], jnp.concatenate(rhs, axis=0), preferred_element_type=F32))
        return out

    def serve_own():
        own = serve(picks(me, me), lambda s, tile: codes[tile] - 32768)
        acc[0], acc[1] = own

    def w_own():
        w_add(c, wdot(cot[...], dsv[...]), True)
        w_done(c)

    def answer(v):
        @pl.when(q_recvs(v))
        def _():
            slots = picks(me - sign * v, me)
            q_from(v).wait_recv()
            parts = serve(slots, lambda s, tile: qrecv[v + R, s].astype(jnp.int32))
            if v in PAIRED:
                hold[v + R] = jnp.where(par == 0, parts[0], parts[1])
                csend[v + R] = jnp.where(par == 0, parts[1], parts[0]).astype(BF16)
                c_copy(v).start()
            else:
                for t in range(2):
                    psend[v + R, t] = parts[t].astype(BF16)
                    p_copy(v, t).start()

    def join(v):
        @pl.when(q_recvs(v))
        def _():
            c_from(v).wait_recv()
            psend[v + R, par] = (hold[v + R] + crecv[v + R].astype(F32)).astype(BF16)
            p_copy(v, par).start()

    def aggregate():
        for v in SERVE_AT:
            u = turn(v)

            @pl.when(q_sends(u))
            def _():
                if v in PAIRED:
                    t = lax.rem(par + u + 2 * R, 2)
                    p_from(u, t).wait_recv()
                    acc[t] += precv[u + R, t].astype(F32)
                else:
                    for t in range(2):
                        p_from(u, t).wait_recv()
                        acc[t] += precv[u + R, t].astype(F32)
        for t in range(2):
            asend[t] = (acc[t] * scale).astype(BF16)
        for f in range(2):
            @pl.when((pos[f] == 0) | (pos[f] == n - 2))
            def _():
                a_start(f)

    def a_start(f):
        for t in range(2):
            for h in range(AP):
                a_copy(f, 0, t, h).start()

    def a_own(f, p):
        @pl.when(pos[f] == p)
        def _():
            a_start(f)

    mixes = (emix, dproj)

    def mix(t, own, value):
        rows = pl.ds(pl.multiple_of(own * ch, ch), ch)
        return jnp.dot(value, mixes[t][rows, :], preferred_element_type=F32)

    def mix_own():
        loads["embed"].wait()
        loads["emix"].wait()
        loads["dproj"].wait()
        for t in range(2):
            acc[t] = mix(t, c, asend[t])

    def a_take(f, p, d, t, h):
        @pl.when(pos[f] == p)
        def _():
            a_from(f, d, t, h).wait_recv()
            if p + 1 < n:
                a_copy(f, d + 1, t, h).start()
            rows = pl.ds(h * arows, arows)
            acc[t, rows, :] += mix(t, owner(f, d), abuf[f, d, t, rows, :])

    def finish(t):
        if t == 0:
            mixed = acc[0]
            hid[...] = (embed[...].astype(F32) + mixed / (1.0 + jnp.exp(-mixed))).astype(BF16)
            stores[0].start()
        else:
            ngrad[...] = acc[1].astype(BF16)
            stores[1].start()

    stores = [
        pltpu.make_async_copy(src, dst, outs.at[i])
        for i, (src, dst) in enumerate(((hid, hid_out), (ngrad, ngrad_out), (wgrad, wgrad_out)))
    ]

    def take(f, p, d, k):
        @pl.when(pos[f] == p)
        def _():
            z_from(f, d, k).wait_recv()
            if p + 1 < n - 1 or (p + 1 == n - 1 and k >= NH):
                z_copy(f, d + 1, k).start()

    def take_help(f):
        @pl.when(pos[f] == n - 2)
        def _():
            help_copy(f).wait_recv()

    def part_own(f):
        @pl.when(pos[f] == n - 2)
        def _():
            hsend[f, 0] = wdot(cot[:hblk], hbuf[f]).astype(BF16)
            part_copy(f, 0).start()

    def part_of(f, d):
        @pl.when(pos[f] == n - 2)
        def _():
            hsend[f, d + 1] = wdot(buf[f, d, :hblk], hbuf[f]).astype(BF16)
            part_copy(f, d + 1).start()

    def w_helped(f, p, d):
        @pl.when(pos[f] == p)
        def _():
            w_add(owner(f, d), wdot(buf[f, d, :hblk], dsv[:hrows]), True)

    def w_rest(f, p, d):
        @pl.when(pos[f] == p)
        def _():
            w_add(owner(f, d), wdot(buf[f, d, hblk:], dsv[hrows:]), p == n - 1)
            if p < n - 1:
                w_done(owner(f, d))

    def w_part(f, d):
        @pl.when(pos[f] == n - 1)
        def _():
            part_copy(f, d).wait_recv()
            w_add(owner(f, d), hrecv[f, d].astype(F32), False)
            w_done(owner(f, d))

    def w_sum():
        w_got().wait_recv()
        wgrad[...] = wacc[pl.ds(pl.multiple_of(me * wrows, wrows), wrows), :]

        @pl.loop(0, nb)
        def _(s):
            @pl.when(s != me)
            def _():
                wgrad[...] += wrecv[s].astype(F32)

        wgrad[...] = wgrad[...] * wscale
        stores[2].start()

    def drain_a():
        for f in range(2):
            for d in range(n - 1):
                @pl.when(a_sends(f, d))
                def _():
                    a_sent(f, d).wait_send()

    def drain_w():
        w_all().wait_send()

    def drain_stores():
        for store in stores:
            store.wait()

    def drain():
        for f in range(2):
            for d in range(n - 1):
                @pl.when(z_sends(f, d, NCH - 1) & (pos[f] + 1 < n - 1))
                def _():
                    z_sent(f, d, 0).wait_send()

                @pl.when(z_sends(f, d, NCH - 1) & (pos[f] + 1 == n - 1))
                def _():
                    z_sent(f, d, NH).wait_send()

                @pl.when(pos[f] == n - 2)
                def _():
                    part_copy(f, d).wait_send()

            @pl.when(pos[f] == n - 1)
            def _():
                help_copy(f).wait_send()
        for u in SEND_ORDER:
            @pl.when(q_sends(u))
            def _():
                q_copy(u).wait_send()

        for v in SERVE_AT:
            @pl.when(q_recvs(v))
            def _():
                p_sent(v).wait_send()
                if v in PAIRED:
                    c_copy(v).wait_send()

    events = []

    def at(time, fn, *args):
        events.append((time, len(events), fn, args))

    def arrives(p, d, k):
        if p == n - 1:
            return k - NH + 1 if d == 0 else (d - 1) * NCH + k + 2
        if p == 1:
            return k + 1 + (NH if k >= LEAD else 0)
        return d * NCH + k + 1

    at(0.5, serve_own)
    at(1.5, w_own)
    for o, time in SERVE_AT.items():
        at(time, answer, o)
    for v, time in JOIN_AT.items():
        at(time, join, v)
    at(GATHER_AT, aggregate)
    at(GATHER_AT + 0.3, mix_own)
    last = 2 * NCH + 2 * n

    def a_arrives(p, d):
        if p == n - 1:
            return GATHER_AT + 2.5 if d == 0 else a_arrives(p - 1, d - 1) + 1.5
        return 2 * NCH + 0.5 + 2 * (d + 1)

    helped_at = LEAD + NH
    for f in range(2):
        at(helped_at + 0.1, take_help, f)
        at(helped_at + 0.5, part_own, f)
        for d in range(n - 2):
            at(max(arrives(n - 2, d, NH - 1), helped_at) + 0.6, part_of, f, d)
        for p in range(1, n):
            for d in range(p):
                for k in range(NH if p == n - 1 else 0, NCH):
                    at(arrives(p, d, k), take, f, p, d, k)
                if p < n - 1:
                    at(arrives(p, d, NH - 1) + 0.7, w_helped, f, p, d)
                at(arrives(p, d, NCH - 1) + 0.4, w_rest, f, p, d)
        for d in range(n - 1):
            known = helped_at if d == 0 else max(arrives(n - 2, d - 1, NH - 1), helped_at)
            at(max(known + 2.5, arrives(n - 1, d, NCH - 1) + 0.5), w_part, f, d)
    for f in range(2):
        for p in range(1, n):
            if p + 1 < n - 1:
                at(max(GATHER_AT, arrives(p, p - 1, NCH - 1)) + 0.35, a_own, f, p)
            for d in range(p):
                for t in range(2):
                    for h in range(AP):
                        when = a_arrives(p, d) + (t * AP + h) / AP
                        at(when if p < n - 1 or d < n - 2 else last + t + h / AP, a_take, f, p, d, t, h)
    at(last + 0.9, finish, 0)
    at(last + WSUM, w_sum)
    at(last + 1.9, finish, 1)
    for i, fn in enumerate((drain, drain_w, drain_a, drain_stores)):
        at(last + 3 + i, fn)
    for _, _, fn, args in sorted(events, key=lambda e: e[:2]):
        fn(*args)


def hand_over(hid_in, ngrad_in, wgrad_in, hid, ngrad, wgrad):
    hid[...] = hid_in[...]
    ngrad[...] = ngrad_in[...]
    wgrad[...] = wgrad_in[...]


def shards(nb, n, cells_next, node_embed, enc_mix, out_cotangent, decoded_saved, dec_proj, tile_source, tile_codes):
    nodes, kk, blkn, blkc = tile_codes.shape
    tiles = nodes * kk
    krows, ch = out_cotangent.shape
    cb = krows // blkc
    width = enc_mix.shape[0]
    wrows = width // nb
    scale = (3.0 / (kk * blkn)) ** 0.5 / 128.0
    wscale = float(krows * nb) ** -0.5
    no = 2 * R + 1
    nn = nodes * blkn
    dma = pltpu.SemaphoreType.DMA
    vm = pltpu.VMEM
    outs = pl.pallas_call(
        functools.partial(kernel, nb, n, scale, wscale),
        name="encode_and_grad",
        out_shape=(
            jax.ShapeDtypeStruct((nn, ch), BF16),
            jax.ShapeDtypeStruct((nn, ch), BF16),
            jax.ShapeDtypeStruct((wrows, ch), F32),
        ),
        in_specs=[pl.BlockSpec(memory_space=pltpu.SMEM)] + [pl.BlockSpec(memory_space=pl.ANY)] * 7,
        out_specs=[pl.BlockSpec(memory_space=pl.ANY)] * 3,
        scratch_shapes=[
            vm((nn, ch), BF16),
            vm((nn, ch), BF16),
            vm((wrows, ch), F32),
            dma((3,)),
            vm((cb, blkc, ch), BF16),
            vm((nn, ch), BF16),
            vm((width, ch), BF16),
            vm((cb, blkc, ch), BF16),
            vm((krows, ch), BF16),
            vm((width, ch), BF16),
            vm((tiles, blkn, blkc), jnp.int32),
            dma((7,)),
            vm((2, n - 1, cb, blkc, ch), BF16),
            vm((2, krows * NH // NCH, ch), BF16),
            vm((2, n - 1, ch, ch), BF16),
            vm((2, n - 1, ch, ch), BF16),
            vm((width, ch), F32),
            vm((width, ch), BF16),
            vm((nb, wrows, ch), BF16),
            vm((no, CAP, blkn, blkc), jnp.int16),
            vm((no, CAP, blkn, blkc), jnp.int16),
            vm((no, 2, nn, ch), BF16),
            vm((no, 2, nn, ch), BF16),
            vm((2, nn, CAP * blkc), BF16),
            vm((2, nn, ch), F32),
            vm((no, nn, ch), BF16),
            vm((no, nn, ch), BF16),
            vm((no, nn, ch), F32),
            vm((2, nn, ch), BF16),
            vm((2, n - 1, 2, nn, ch), BF16),
            dma((2, n - 1)),
            dma((n - 1, NCH)),
            dma((2,)),
            dma((2,)),
            dma((2, n - 1)),
            dma((2, n - 1)),
            dma((1,)),
            dma((1,)),
            dma((no,)),
            dma((no,)),
            dma((no,)),
            dma((no, 2)),
            dma((2, n - 1)),
            dma((n - 1, 2, AP)),
            dma((no,)),
            dma((no,)),
        ],
        compiler_params=pltpu.CompilerParams(
            collective_id=0, has_side_effects=True, vmem_limit_bytes=56 * 1024 * 1024
        ),
    )(
        tile_source,
        cells_next.reshape(cb, blkc, ch), node_embed, enc_mix,
        out_cotangent.reshape(cb, blkc, ch), decoded_saved, dec_proj,
        tile_codes.reshape(tiles, blkn, blkc),
    )
    return pl.pallas_call(
        hand_over,
        name="hand_over",
        out_shape=tuple(jax.ShapeDtypeStruct(x.shape, x.dtype) for x in outs),
        in_specs=[pl.BlockSpec(memory_space=vm)] * 3,
        out_specs=[pl.BlockSpec(memory_space=vm)] * 3,
    )(*outs)


def solution(mesh):
    nb, n = mesh.shape["band"], mesh.shape["chan"]
    in_specs = (
        P("band", "chan"),
        P("band", "chan"),
        P(None, "chan"),
        P("band", "chan"),
        P("band", "chan"),
        P(None, "chan"),
        P(),
        P("band", None, None, None),
    )
    out_specs = (P("band", "chan"), P("band", "chan"), P("band", "chan"))
    return jax.shard_map(
        functools.partial(shards, nb, n),
        mesh=mesh,
        in_specs=in_specs,
        out_specs=out_specs,
        check_vma=False,
    )
```

```python
import functools

import jax
import jax.numpy as jnp
from jax import lax
from jax.experimental import pallas as pl
from jax.experimental.pallas import tpu as pltpu
from jax.sharding import PartitionSpec as P

R = 3
CAP = 8
SEND_ORDER = [3, 2, -2, -1, -3, 1]
MATE = -1
PAIRED = {v for v in range(-R, R + 1) if v not in (0, MATE) and -v - 1 not in (0, MATE) and -R <= -v - 1 <= R}
SERVE_AT = {-3: 2.6, 2: 4.6, -2: 6.6, 1: 7.6, 3: 7.7, -1: 7.8}
JOIN_AT = {-3: 4.7, 2: 4.8, -2: 7.9, 1: 8.0}
GATHER_AT = 12.3
NCH = 8
NH = 6
LEAD = 4
AP = 2
WSUM = 2
MESH = pl.DeviceIdType.MESH
F32 = jnp.float32
BF16 = jnp.bfloat16


def kernel(
    nb, n, scale, wscale,
    src_in, cells_in, embed_in, emix_in, cot_in, dsv_in, dproj_in, codes_in,
    hid_out, ngrad_out, wgrad_out,
    hid, ngrad, wgrad, outs,
    src_of, cells, embed, emix, cot, dsv, dproj, codes, ls,
    buf, hbuf, hsend, hrecv, wacc, wsend, wrecv, qsend, qrecv, psend, precv, lhs, acc,
    csend, crecv, hold,
    asend, abuf,
    zs, zr, hs, hr, hps, hpr, ws, wr, qs, qr, ps, pr, zas, zar, cs, cr,
):
    me = lax.axis_index("band")
    c = lax.axis_index("chan")
    kk = src_of.shape[1]
    nodes = codes.shape[0] // kk
    blkrows = cells.shape[1]
    ch = embed.shape[1]
    cb = cot.shape[0]
    krows = cb * blkrows
    cblk = cb // NCH
    hrows = NH * cblk * blkrows
    hblk = NH * cblk
    wrows = wrecv.shape[1]
    per = ch // wrows

    def rc(src, dst, ss, rs, dev):
        return pltpu.make_async_remote_copy(
            src_ref=src, dst_ref=dst, send_sem=ss, recv_sem=rs, device_id=dev, device_id_type=MESH
        )

    pos = [c, n - 1 - c]
    nxt = [lax.rem(c + 1, n), lax.rem(c + n - 1, n)]
    prv = [nxt[1], nxt[0]]

    def owner(f, d):
        return c - 1 - d if f == 0 else c + 1 + d

    def z_sends(f, d, k):
        ok = (pos[f] + 1 < n) & (pos[f] - d >= 0)
        return ok if k >= NH else ok & (pos[f] + 1 < n - 1)

    def slot_at(f, d, ahead):
        return d if f == 0 else d + c - ahead

    def z_copy(f, d, k):
        rows = pl.ds(k * cblk, cblk)
        src = cot.at[rows] if d == 0 else buf.at[f, d - 1, rows]
        return rc(src, buf.at[f, d, rows], zs.at[f, d], zr.at[slot_at(f, d, 1), k], {"chan": nxt[f]})

    def z_from(f, d, k):
        rows = pl.ds(k * cblk, cblk)
        dst = buf.at[f, d, rows]
        return rc(dst, dst, zs.at[f, d], zr.at[slot_at(f, d, 0), k], {"chan": nxt[f]})

    def z_sent(f, d, first):
        rows = pl.ds(first * cblk, cb - first * cblk)
        dst = buf.at[f, d, rows]
        return rc(dst, dst, zs.at[f, d], zr.at[0, 0], {"chan": nxt[f]})

    def a_sends(f, d):
        return (pos[f] + 1 < n) & (pos[f] - d >= 0)

    arows = embed.shape[0] // AP

    def a_copy(f, d, t, h):
        rows = pl.ds(h * arows, arows)
        src = asend.at[t, rows] if d == 0 else abuf.at[f, d - 1, t, rows]
        return rc(src, abuf.at[f, d, t, rows], zas.at[f, d], zar.at[slot_at(f, d, 1), t, h], {"chan": nxt[f]})

    def a_from(f, d, t, h):
        dst = abuf.at[f, d, t, pl.ds(h * arows, arows)]
        return rc(dst, dst, zas.at[f, d], zar.at[slot_at(f, d, 0), t, h], {"chan": nxt[f]})

    def a_sent(f, d):
        dst = abuf.at[f, d]
        return rc(dst, dst, zas.at[f, d], zar.at[0, 0, 0], {"chan": nxt[f]})

    def help_copy(f):
        return rc(dsv.at[pl.ds(0, hrows)], hbuf.at[f], hs.at[f], hr.at[f], {"chan": prv[f]})

    def part_copy(f, e):
        return rc(hsend.at[f, e], hrecv.at[f, e], hps.at[f, e], hpr.at[f, e], {"chan": nxt[f]})

    par = lax.rem(me, 2)
    sign = 1 - 2 * par
    mate = me + sign

    def turn(u):
        return u if u % 2 == 0 else -u

    def picks(band, wanted):
        low = wanted * cb
        bits = (max(cb, kk) - 1).bit_length()
        one = jnp.int32(1)
        zero = jnp.int32(0)
        seen, block, place, part = zero, zero, zero, zero
        unit, flag = one, one
        for m in range(nodes):
            for k in range(kk):
                off = src_of[band * nodes + m, k] - low
                hit = (off >= 0) & (off < cb)
                block += jnp.where(hit, off * unit, 0)
                place += jnp.where(hit, k * unit, 0)
                part += jnp.where(hit, m * flag, 0)
                seen += jnp.where(hit, 1, 0)
                unit = jnp.where(hit, unit * 2**bits, unit)
                flag = jnp.where(hit, flag * nodes, flag)

        def field(word, s, size):
            return (word >> (size * s)) & (2**size - 1)

        mbits = (nodes - 1).bit_length()
        slots = []
        for s in range(CAP):
            m = field(part, s, mbits)
            keeps = [jnp.where((m == i) & (s < seen), 1.0, 0.0) for i in range(nodes)]
            slots.append((m * kk + field(place, s, bits), field(block, s, bits), keeps))
        return slots

    def q_copy(u):
        v = turn(u)
        to = lax.rem(me + sign * u + nb, nb)
        return rc(qsend.at[u + R], qrecv.at[v + R], qs.at[u + R], qr.at[v + R], {"band": to})

    def q_from(v):
        return rc(qsend.at[v + R], qrecv.at[v + R], qs.at[v + R], qr.at[v + R], {"band": me})

    def c_copy(v):
        w = -v - 1
        return rc(csend.at[v + R], crecv.at[w + R], cs.at[v + R], cr.at[w + R], {"band": mate})

    def c_from(v):
        return rc(csend.at[v + R], crecv.at[v + R], cs.at[v + R], cr.at[v + R], {"band": mate})

    def p_copy(v, t):
        u = turn(v)
        to = lax.rem(me - sign * v + nb, nb)
        return rc(psend.at[v + R, t], precv.at[u + R, t], ps.at[v + R], pr.at[u + R, t], {"band": to})

    def p_sent(v):
        src = psend.at[v + R, 0] if v in PAIRED else psend.at[v + R]
        return rc(src, src, ps.at[v + R], ps.at[v + R], {"band": me})

    def p_from(u, t):
        return rc(psend.at[u + R, t], precv.at[u + R, t], ps.at[u + R], pr.at[u + R, t], {"band": me})

    def q_sends(u):
        return (me + sign * u >= 0) & (me + sign * u < nb)

    def q_recvs(v):
        return (me - sign * v >= 0) & (me - sign * v < nb)

    def w_copy(s):
        rows = pl.ds(pl.multiple_of(s * wrows, wrows), wrows)
        return rc(wsend.at[rows], wrecv.at[me], ws.at[0], wr.at[0], {"band": s})

    def w_all():
        rows = wsend.at[pl.ds(0, (nb - 1) * wrows)]
        return rc(rows, rows, ws.at[0], ws.at[0], {"band": me})

    def w_got():
        blocks = wrecv.at[pl.ds(0, nb - 1)]
        return rc(blocks, blocks, wr.at[0], wr.at[0], {"band": me})

    def wdot(a, b):
        a = a.reshape(-1, ch)
        return lax.dot_general(a, b, (((0,), (0,)), ((), ())), preferred_element_type=F32)

    def w_done(own):
        rows = pl.ds(pl.multiple_of(own * ch, ch), ch)
        wsend[rows, :] = wacc[rows, :].astype(BF16)

        @pl.loop(0, per)
        def _(j):
            s = own * per + j

            @pl.when(s != me)
            def _():
                w_copy(s).start()

    def w_add(own, value, first):
        rows = pl.ds(pl.multiple_of(own * ch, ch), ch)
        if first:
            wacc[rows, :] = value
        else:
            wacc[rows, :] += value

    loads = {
        name: pltpu.make_async_copy(src, dst, ls.at[i])
        for i, (name, src, dst) in enumerate(
            (
                ("cot", cot_in, cot),
                ("codes", codes_in, codes),
                ("dsv", dsv_in, dsv),
                ("cells", cells_in, cells),
                ("emix", emix_in, emix),
                ("dproj", dproj_in, dproj),
                ("embed", embed_in, embed),
                ("src", src_in, src_of),
            )
        )
    }
    for load_in in loads.values():
        load_in.start()

    barrier = pltpu.get_barrier_semaphore()

    @pl.loop(1, nb)
    def _(j):
        pl.semaphore_signal(
            barrier, inc=1, device_id={"band": lax.rem(me + j, nb)}, device_id_type=MESH
        )

    for f in range(2):
        @pl.when(pos[f] + 1 < n)
        def _():
            pl.semaphore_signal(barrier, inc=1, device_id={"chan": nxt[f]}, device_id_type=MESH)

    beside = jnp.where(c > 0, 1, 0) + jnp.where(c < n - 1, 1, 0)
    pl.semaphore_wait(barrier, nb - 1 + beside)

    loads["cot"].wait()
    loads["dsv"].wait()

    def start_own(k):
        for f in range(2):
            @pl.when(z_sends(f, 0, k))
            def _():
                z_copy(f, 0, k).start()

    for k in range(LEAD):
        start_own(k)
    for f in range(2):
        @pl.when(pos[f] == n - 1)
        def _():
            help_copy(f).start()
    for k in range(LEAD, NCH):
        start_own(k)

    loads["src"].wait()
    loads["codes"].wait()
    for u in SEND_ORDER:
        @pl.when(q_sends(u))
        def _():
            for s, (tile, _, _) in enumerate(picks(me, me + sign * u)):
                qsend[u + R, s] = (codes[tile] - 32768).astype(jnp.int16)
            q_copy(u).start()

    loads["cells"].wait()

    def serve(slots, load):
        for s, (tile, _, keeps) in enumerate(slots):
            word = load(s, tile)
            cols = pl.ds(s * blkrows, blkrows)
            enc = ((word & 255) - 128).astype(F32)
            dec = (word >> 8).astype(F32)
            for m in range(nodes):
                keep = keeps[m]
                rows = pl.ds(m * blkrows, blkrows)
                lhs[0, rows, cols] = (enc * keep).astype(BF16)
                lhs[1, rows, cols] = (dec * keep).astype(BF16)
        out = []
        for t, src in enumerate((cells, cot)):
            rhs = [src[block] for _, block, _ in slots]
            out.append(jnp.dot(lhs[t], jnp.concatenate(rhs, axis=0), preferred_element_type=F32))
        return out

    def serve_own():
        own = serve(picks(me, me), lambda s, tile: codes[tile] - 32768)
        acc[0], acc[1] = own

    def w_own():
        w_add(c, wdot(cot[...], dsv[...]), True)
        w_done(c)

    def answer(v):
        @pl.when(q_recvs(v))
        def _():
            slots = picks(me - sign * v, me)
            q_from(v).wait_recv()
            parts = serve(slots, lambda s, tile: qrecv[v + R, s].astype(jnp.int32))
            if v in PAIRED:
                hold[v + R] = jnp.where(par == 0, parts[0], parts[1])
                csend[v + R] = jnp.where(par == 0, parts[1], parts[0]).astype(BF16)
                c_copy(v).start()
            else:
                for t in range(2):
                    psend[v + R, t] = parts[t].astype(BF16)
                    p_copy(v, t).start()

    def join(v):
        @pl.when(q_recvs(v))
        def _():
            c_from(v).wait_recv()
            psend[v + R, par] = (hold[v + R] + crecv[v + R].astype(F32)).astype(BF16)
            p_copy(v, par).start()

    def aggregate():
        for v in SERVE_AT:
            u = turn(v)

            @pl.when(q_sends(u))
            def _():
                if v in PAIRED:
                    t = lax.rem(par + u + 2 * R, 2)
                    p_from(u, t).wait_recv()
                    acc[t] += precv[u + R, t].astype(F32)
                else:
                    for t in range(2):
                        p_from(u, t).wait_recv()
                        acc[t] += precv[u + R, t].astype(F32)
        for t in range(2):
            asend[t] = (acc[t] * scale).astype(BF16)
        for f in range(2):
            @pl.when((pos[f] == 0) | (pos[f] == n - 2))
            def _():
                a_start(f)

    def a_start(f):
        for t in range(2):
            for h in range(AP):
                a_copy(f, 0, t, h).start()

    def a_own(f, p):
        @pl.when(pos[f] == p)
        def _():
            a_start(f)

    mixes = (emix, dproj)

    def mix(t, own, value):
        rows = pl.ds(pl.multiple_of(own * ch, ch), ch)
        return jnp.dot(value, mixes[t][rows, :], preferred_element_type=F32)

    def mix_own():
        loads["embed"].wait()
        loads["emix"].wait()
        loads["dproj"].wait()
        for t in range(2):
            acc[t] = mix(t, c, asend[t])

    def a_take(f, p, d, t, h):
        @pl.when(pos[f] == p)
        def _():
            a_from(f, d, t, h).wait_recv()
            if p + 1 < n:
                a_copy(f, d + 1, t, h).start()
            rows = pl.ds(h * arows, arows)
            acc[t, rows, :] += mix(t, owner(f, d), abuf[f, d, t, rows, :])

    def finish(t):
        if t == 0:
            mixed = acc[0]
            hid[...] = (embed[...].astype(F32) + mixed / (1.0 + jnp.exp(-mixed))).astype(BF16)
            stores[0].start()
        else:
            ngrad[...] = acc[1].astype(BF16)
            stores[1].start()

    stores = [
        pltpu.make_async_copy(src, dst, outs.at[i])
        for i, (src, dst) in enumerate(((hid, hid_out), (ngrad, ngrad_out), (wgrad, wgrad_out)))
    ]

    def take(f, p, d, k):
        @pl.when(pos[f] == p)
        def _():
            z_from(f, d, k).wait_recv()
            if p + 1 < n - 1 or (p + 1 == n - 1 and k >= NH):
                z_copy(f, d + 1, k).start()

    def take_help(f):
        @pl.when(pos[f] == n - 2)
        def _():
            help_copy(f).wait_recv()

    def part_own(f):
        @pl.when(pos[f] == n - 2)
        def _():
            hsend[f, 0] = wdot(cot[:hblk], hbuf[f]).astype(BF16)
            part_copy(f, 0).start()

    def part_of(f, d):
        @pl.when(pos[f] == n - 2)
        def _():
            hsend[f, d + 1] = wdot(buf[f, d, :hblk], hbuf[f]).astype(BF16)
            part_copy(f, d + 1).start()

    def w_helped(f, p, d):
        @pl.when(pos[f] == p)
        def _():
            w_add(owner(f, d), wdot(buf[f, d, :hblk], dsv[:hrows]), True)

    def w_rest(f, p, d):
        @pl.when(pos[f] == p)
        def _():
            w_add(owner(f, d), wdot(buf[f, d, hblk:], dsv[hrows:]), p == n - 1)
            if p < n - 1:
                w_done(owner(f, d))

    def w_part(f, d):
        @pl.when(pos[f] == n - 1)
        def _():
            part_copy(f, d).wait_recv()
            w_add(owner(f, d), hrecv[f, d].astype(F32), False)
            w_done(owner(f, d))

    def w_sum():
        w_got().wait_recv()
        wgrad[...] = wacc[pl.ds(pl.multiple_of(me * wrows, wrows), wrows), :]

        @pl.loop(0, nb)
        def _(s):
            @pl.when(s != me)
            def _():
                wgrad[...] += wrecv[s].astype(F32)

        wgrad[...] = wgrad[...] * wscale
        stores[2].start()

    def drain_a():
        for f in range(2):
            for d in range(n - 1):
                @pl.when(a_sends(f, d))
                def _():
                    a_sent(f, d).wait_send()

    def drain_w():
        w_all().wait_send()

    def drain_stores():
        for store in stores:
            store.wait()

    def drain():
        for f in range(2):
            for d in range(n - 1):
                @pl.when(z_sends(f, d, NCH - 1) & (pos[f] + 1 < n - 1))
                def _():
                    z_sent(f, d, 0).wait_send()

                @pl.when(z_sends(f, d, NCH - 1) & (pos[f] + 1 == n - 1))
                def _():
                    z_sent(f, d, NH).wait_send()

                @pl.when(pos[f] == n - 2)
                def _():
                    part_copy(f, d).wait_send()

            @pl.when(pos[f] == n - 1)
            def _():
                help_copy(f).wait_send()
        for u in SEND_ORDER:
            @pl.when(q_sends(u))
            def _():
                q_copy(u).wait_send()

        for v in SERVE_AT:
            @pl.when(q_recvs(v))
            def _():
                p_sent(v).wait_send()
                if v in PAIRED:
                    c_copy(v).wait_send()

    events = []

    def at(time, fn, *args):
        events.append((time, len(events), fn, args))

    def arrives(p, d, k):
        if p == n - 1:
            return k - NH + 1 if d == 0 else (d - 1) * NCH + k + 2
        if p == 1:
            return k + 1 + (NH if k >= LEAD else 0)
        return d * NCH + k + 1

    at(0.5, serve_own)
    at(1.5, w_own)
    for o, time in SERVE_AT.items():
        at(time, answer, o)
    for v, time in JOIN_AT.items():
        at(time, join, v)
    at(GATHER_AT, aggregate)
    at(GATHER_AT + 0.3, mix_own)
    last = 2 * NCH + 2 * n

    def a_arrives(p, d):
        if p == n - 1:
            return GATHER_AT + 2.5 if d == 0 else a_arrives(p - 1, d - 1) + 1.5
        return 2 * NCH + 0.5 + 2 * (d + 1)

    helped_at = LEAD + NH
    for f in range(2):
        at(helped_at + 0.1, take_help, f)
        at(helped_at + 0.5, part_own, f)
        for d in range(n - 2):
            at(max(arrives(n - 2, d, NH - 1), helped_at) + 0.6, part_of, f, d)
        for p in range(1, n):
            for d in range(p):
                for k in range(NH if p == n - 1 else 0, NCH):
                    at(arrives(p, d, k), take, f, p, d, k)
                if p < n - 1:
                    at(arrives(p, d, NH - 1) + 0.7, w_helped, f, p, d)
                at(arrives(p, d, NCH - 1) + 0.4, w_rest, f, p, d)
        for d in range(n - 1):
            known = helped_at if d == 0 else max(arrives(n - 2, d - 1, NH - 1), helped_at)
            at(max(known + 2.5, arrives(n - 1, d, NCH - 1) + 0.5), w_part, f, d)
    for f in range(2):
        for p in range(1, n):
            if p + 1 < n - 1:
                at(max(GATHER_AT, arrives(p, p - 1, NCH - 1)) + 0.35, a_own, f, p)
            for d in range(p):
                for t in range(2):
                    for h in range(AP):
                        when = a_arrives(p, d) + (t * AP + h) / AP
                        at(when if p < n - 1 or d < n - 2 else last + t + h / AP, a_take, f, p, d, t, h)
    at(last + 0.9, finish, 0)
    at(last + WSUM, w_sum)
    at(last + 1.9, finish, 1)
    for i, fn in enumerate((drain, drain_w, drain_a, drain_stores)):
        at(last + 3 + i, fn)
    for _, _, fn, args in sorted(events, key=lambda e: e[:2]):
        fn(*args)


def hand_over(hid_in, ngrad_in, wgrad_in, hid, ngrad, wgrad):
    hid[...] = hid_in[...]
    ngrad[...] = ngrad_in[...]
    wgrad[...] = wgrad_in[...]


def shards(nb, n, cells_next, node_embed, enc_mix, out_cotangent, decoded_saved, dec_proj, tile_source, tile_codes):
    nodes, kk, blkn, blkc = tile_codes.shape
    tiles = nodes * kk
    krows, ch = out_cotangent.shape
    cb = krows // blkc
    width = enc_mix.shape[0]
    wrows = width // nb
    scale = (3.0 / (kk * blkn)) ** 0.5 / 128.0
    wscale = float(krows * nb) ** -0.5
    no = 2 * R + 1
    nn = nodes * blkn
    dma = pltpu.SemaphoreType.DMA
    vm = pltpu.VMEM
    outs = pl.pallas_call(
        functools.partial(kernel, nb, n, scale, wscale),
        name="encode_and_grad",
        out_shape=(
            jax.ShapeDtypeStruct((nn, ch), BF16),
            jax.ShapeDtypeStruct((nn, ch), BF16),
            jax.ShapeDtypeStruct((wrows, ch), F32),
        ),
        in_specs=[pl.BlockSpec(memory_space=pl.ANY)] * 8,
        out_specs=[pl.BlockSpec(memory_space=pl.ANY)] * 3,
        scratch_shapes=[
            vm((nn, ch), BF16),
            vm((nn, ch), BF16),
            vm((wrows, ch), F32),
            dma((3,)),
            pltpu.SMEM(tile_source.shape, jnp.int32),
            vm((cb, blkc, ch), BF16),
            vm((nn, ch), BF16),
            vm((width, ch), BF16),
            vm((cb, blkc, ch), BF16),
            vm((krows, ch), BF16),
            vm((width, ch), BF16),
            vm((tiles, blkn, blkc), jnp.int32),
            dma((8,)),
            vm((2, n - 1, cb, blkc, ch), BF16),
            vm((2, krows * NH // NCH, ch), BF16),
            vm((2, n - 1, ch, ch), BF16),
            vm((2, n - 1, ch, ch), BF16),
            vm((width, ch), F32),
            vm((width, ch), BF16),
            vm((nb, wrows, ch), BF16),
            vm((no, CAP, blkn, blkc), jnp.int16),
            vm((no, CAP, blkn, blkc), jnp.int16),
            vm((no, 2, nn, ch), BF16),
            vm((no, 2, nn, ch), BF16),
            vm((2, nn, CAP * blkc), BF16),
            vm((2, nn, ch), F32),
            vm((no, nn, ch), BF16),
            vm((no, nn, ch), BF16),
            vm((no, nn, ch), F32),
            vm((2, nn, ch), BF16),
            vm((2, n - 1, 2, nn, ch), BF16),
            dma((2, n - 1)),
            dma((n - 1, NCH)),
            dma((2,)),
            dma((2,)),
            dma((2, n - 1)),
            dma((2, n - 1)),
            dma((1,)),
            dma((1,)),
            dma((no,)),
            dma((no,)),
            dma((no,)),
            dma((no, 2)),
            dma((2, n - 1)),
            dma((n - 1, 2, AP)),
            dma((no,)),
            dma((no,)),
        ],
        compiler_params=pltpu.CompilerParams(
            collective_id=0, has_side_effects=True, vmem_limit_bytes=56 * 1024 * 1024
        ),
    )(
        tile_source,
        cells_next.reshape(cb, blkc, ch), node_embed, enc_mix,
        out_cotangent.reshape(cb, blkc, ch), decoded_saved, dec_proj,
        tile_codes.reshape(tiles, blkn, blkc),
    )
    return pl.pallas_call(
        hand_over,
        name="hand_over",
        out_shape=tuple(jax.ShapeDtypeStruct(x.shape, x.dtype) for x in outs),
        in_specs=[pl.BlockSpec(memory_space=vm)] * 3,
        out_specs=[pl.BlockSpec(memory_space=vm)] * 3,
    )(*outs)


def solution(mesh):
    nb, n = mesh.shape["band"], mesh.shape["chan"]
    in_specs = (
        P("band", "chan"),
        P("band", "chan"),
        P(None, "chan"),
        P("band", "chan"),
        P("band", "chan"),
        P(None, "chan"),
        P(),
        P("band", None, None, None),
    )
    out_specs = (P("band", "chan"), P("band", "chan"), P("band", "chan"))
    return jax.shard_map(
        functools.partial(shards, nb, n),
        mesh=mesh,
        in_specs=in_specs,
        out_specs=out_specs,
        check_vma=False,
    )
```
